128 devices in a mesh: rows: 8 (over x, y_lo), tensor: 16 (over z, y_hi, core).
Axes of the slice: x: 4, y: 4 (y_hi: 2, y_lo: 2; y = y_hi * 2 + y_lo), z: 4, core: 2. Of those that a mesh axis runs over, the one named last changes fastest.
Arguments:
- hidden: bfloat16 [2048, 28672], P('rows', 'tensor'), may hold values from -6 to 6
- down_weight: bfloat16 [28672, 8192], P('tensor', 'rows'), may hold values from -0.046875 to 0.046875
- low_feat: bfloat16 [2048, 8192], P('rows', 'tensor'), may hold values from -6 to 6
- mid_feat: bfloat16 [2048, 8192], P('rows', 'tensor'), may hold values from -6 to 6
- draft_rows: int32 [2048], replicated, may hold values from 0 to 2047, each once
- join_weight: bfloat16 [3, 8192, 8192], P(None, 'tensor', 'rows'), may hold values from -0.0390625 to 0.0390625
- cotangent: bfloat16 [2048, 8192], P('tensor', 'rows'), may hold values from -0.1796875 to 0.1796875
Outputs:
- joined: bfloat16 [2048, 8192], P('tensor', 'rows')
- join_grad: float32 [3, 8192, 8192], P(None, 'tensor', 'rows')
The draws below stay inside these ranges and needn't reach their ends.
Inputs may be any that keep to these rules, and one draw needn't show every extreme that they name: draft_rows is a permutation of the 2048 target tokens.
All inputs are finite; a program needn't handle non-finite values.
Results may differ from the reference program's by a relative error of at most 0.0038.
Values may be sent and summed in bfloat16 or wider, within the bound.
A program may use at most 128 MiB of HBM per device.

```python
import jax
import jax.numpy as jnp

D = 8192
FF = 28672
TOKENS = 2048


def with_spikes(drawn, rng, source, target, shards_of, factor):
    def block_of(axis_at):
        return (jnp.arange(drawn.shape[axis_at]) // (drawn.shape[axis_at] // shards_of)).reshape((-1,) + (1,) * (drawn.ndim - 1 - axis_at))

    one_side = jax.random.permutation(rng, shards_of)[block_of(target)]
    far = (block_of(target) + shards_of // 2) % shards_of
    return jnp.where((block_of(source) == one_side) | (block_of(source) == far), factor * drawn, drawn)


def shard_levels(rng, shape, shards, low, high):
    factor_of, own = 1.0, jax.random.fold_in(rng, 6)
    for position, shards_of in shards:
        steps = jnp.exp(jax.random.uniform(jax.random.fold_in(own, position), (shards_of,), jnp.float32, low / len(shards), high / len(shards)))
        factor_of = factor_of * jnp.repeat(steps, shape[position] // shards_of).reshape([-1 if axis == position else 1 for axis in range(len(shape))])
    return factor_of


def scatter_about(stream_key, shape, scale, most, cuts=(), dtype=jnp.bfloat16):
    loudness = shard_levels(stream_key, shape, cuts, -0.22, 0.18) if cuts else 1.0
    array = jax.random.normal(stream_key, shape, jnp.float32) * scale * loudness
    return jnp.minimum(jnp.maximum(array, -most), most).astype(dtype)


def gaussian_with(stream_key, shape, width, bound, shards, heavy, dtype=jnp.bfloat16):
    result = width * jax.random.normal(stream_key, shape, jnp.float32)
    if shards:
        result = result * shard_levels(stream_key, shape, shards, -0.22, 0.18)
    return jnp.clip(with_spikes(result, jax.random.fold_in(stream_key, 3), *heavy), -bound, bound).astype(dtype)


def setup_inputs(seed: int = 0) -> dict:
    seeds = jax.random.split(jax.random.key(seed), 8)
    return {
        "hidden": scatter_about(seeds[0], (TOKENS, FF), 1.0, 6.0, ((0, 8), (1, 16))),
        "down_weight": gaussian_with(seeds[1], (FF, D), FF ** -0.5, 0.046875, ((0, 16), (1, 8)), (0, 1, 16, 2.0)),
        "low_feat": scatter_about(seeds[2], (TOKENS, D), 1.0, 6.0, ((0, 8), (1, 16))),
        "mid_feat": scatter_about(seeds[3], (TOKENS, D), 1.0, 6.0, ((0, 8), (1, 16))),
        "draft_rows": jax.random.permutation(seeds[4], TOKENS).astype(jnp.int32),
        "join_weight": scatter_about(seeds[5], (3, D, D), (3 * D) ** -0.5, 0.0390625, ((1, 16), (2, 8))),
        "cotangent": scatter_about(seeds[6], (TOKENS, D), 0.03, 0.1796875, ((0, 16), (1, 8))),
    }


def reference(hidden, down_weight, low_feat, mid_feat, draft_rows, join_weight, cotangent):
    high_feat = jnp.dot(hidden, down_weight, preferred_element_type=jnp.float32).astype(jnp.bfloat16)
    picks = draft_rows.astype(jnp.int32)
    features = (low_feat, mid_feat, high_feat)
    joined = jnp.zeros((TOKENS, D), jnp.float32)
    grads = []
    for index in range(3):
        ordered = jnp.take(features[index], picks, axis=0)
        joined = joined + jnp.dot(ordered, join_weight[index], preferred_element_type=jnp.float32)
        grads.append(jnp.dot(ordered.T, cotangent, preferred_element_type=jnp.float32))
    return joined.astype(jnp.bfloat16), jnp.stack(grads, axis=0)
```

```python
import jax
import jax.numpy as jnp
from jax import lax
from jax.experimental import pallas as pl
from jax.experimental.pallas import tpu as pltpu
from jax.sharding import Mesh
from jax.sharding import PartitionSpec as P

AXES = ("x", "yl", "z", "yh", "c")
ROWS = ("x", "yl")
TENSOR = ("z", "yh", "c")
MESH = pl.DeviceIdType.MESH
F32, BF16 = jnp.float32, jnp.bfloat16
DX = (0, 3, 1, 0, 3, 1, 2, 2)
DY = (0, 0, 0, 1, 1, 1, 0, 1)
CUT, MID = 96, 176


def mod4(i):
    return lax.rem(i + 8, 4)


class Copies:
    def __init__(self, send_sems, recv_sems):
        self.send_sems, self.recv_sems, self.made, self.open = send_sems, recv_sems, 0, []

    def send(self, src, dst, to):
        k = self.made
        self.made += 1
        copy = pltpu.make_async_remote_copy(
            src_ref=src,
            dst_ref=dst,
            send_sem=self.send_sems.at[k],
            recv_sem=self.recv_sems.at[k],
            device_id=to,
            device_id_type=MESH,
        )
        copy.start()
        self.open.append(copy)
        return copy

    def drain(self):
        for copy in self.open:
            copy.wait_send()
        self.open = []


class RowGather:
    def __init__(self, copies, buf, src, right, left, across):
        self.send, self.buf, self.src = copies.send, buf, src
        self.right, self.left, self.across = right, left, across

    def own(self):
        b = self.buf
        self.p = self.send(self.src, b.at[3], self.across)
        self.r = self.send(self.src, b.at[1], self.right)
        self.l = self.send(self.src, b.at[2], self.left)

    def near(self):
        b = self.buf
        self.p.wait_recv()
        self.pr = self.send(b.at[3, CUT:], b.at[4, CUT:], self.right)
        self.pl = self.send(b.at[3, CUT:], b.at[5, CUT:], self.left)
        self.r.wait_recv()
        self.fr = self.send(b.at[1, :128], b.at[6, :128], self.right)
        self.yl = self.send(b.at[1, :CUT], b.at[4, :CUT], self.across)
        self.l.wait_recv()
        self.fl = self.send(b.at[2, 128:], b.at[6, 128:], self.left)
        self.yr = self.send(b.at[2, :CUT], b.at[5, :CUT], self.across)

    def far(self):
        b = self.buf
        self.pr.wait_recv()
        self.fpr = self.send(b.at[4, CUT:MID], b.at[7, CUT:MID], self.right)
        self.pl.wait_recv()
        self.fpl = self.send(b.at[5, MID:], b.at[7, MID:], self.left)

    def sides(self):
        self.yl.wait_recv()
        self.yr.wait_recv()

    def opposite(self):
        b = self.buf
        self.fr.wait_recv()
        self.yo = self.send(b.at[6, :CUT], b.at[7, :CUT], self.across)
        self.fl.wait_recv()

    def last(self):
        self.yo.wait_recv()
        self.fpr.wait_recv()
        self.fpl.wait_recv()


def kernel(
    dr_hbm, hid, w, low, mid, wj, cot,
    joined, ordered_out, cot_out,
    dr, hid_all, w4, lm_all, pq, drecv, drecv2, zr, yr, hp, high, ordered, sel, wjv,
    sb, rb, ys, yr2, cot_all, send_sems, recv_sems, high_send, high_recv, local,
):
    x, yl, z, yh, c = (lax.axis_index(a) for a in AXES)
    right, left = (mod4(x + 1), yl, z, yh, c), (mod4(x - 1), yl, z, yh, c)
    across = (x, 1 - yl, z, yh, c)
    up, down = (x, yl, mod4(z + 1), yh, c), (x, yl, mod4(z - 1), yh, c)
    far_y, core = (x, yl, z, 1 - yh, c), (x, yl, z, yh, 1 - c)
    copies = Copies(send_sems, recv_sems)
    quarter = w4.shape[2]
    half = 2 * quarter
    nlocal = [0]

    def load(src, dst):
        k = nlocal[0]
        nlocal[0] += 1
        copy = pltpu.make_async_copy(src, dst, local.at[k])
        copy.start()
        return copy

    def cb(dz, y, core_at):
        return cot_all.at[mod4(z + dz) * 4 + y * 2 + core_at]

    own_cot = cb(0, yh, c)
    cy = copies.send(cot, own_cot, far_y)
    hidden = RowGather(copies, hid_all, hid, right, left, across)
    hidden.own()
    loads = [load(hid, hid_all.at[0])]
    for j in range(4):
        at = pl.multiple_of(lax.rem(c + (1 if j < 2 else 0), 2) * half + (j % 2) * quarter, quarter)
        loads.append(load(w.at[:, pl.ds(at, quarter)], w4.at[j]))
    cot_up, cot_down, to_core = copies.send(cot, own_cot, up), copies.send(cot, own_cot, down), []
    to_core.append(copies.send(cot, own_cot, core))
    late = [load(cot, own_cot), load(low, lm_all.at[0, :, 0 : low.shape[1]])]
    late.append(load(mid, lm_all.at[0, :, low.shape[1] :]))
    late.append(load(dr_hbm, dr))
    depth = low.shape[1]
    for k in range(3):
        for d in range(2):
            late.append(
                load(wj.at[k, :, d * half : (d + 1) * half], wjv.at[d, k * depth : (k + 1) * depth])
            )
    for copy in loads:
        copy.wait()

    def project(first, stop, which):
        def body(i, _):
            s, j = first + i // 2, i % 2
            pq[which, s, j] = jnp.dot(hid_all[s], w4[which * 2 + j], preferred_element_type=F32)
            return 0

        lax.fori_loop(0, 2 * (stop - first), body, 0)

    to_pair = {}

    def product(first, stop):
        project(first, stop, 0)
        for s in range(first, stop):
            to_pair[s] = copies.send(pq.at[0, s], drecv.at[s], core)
        project(first, stop, 1)

    def pair_sum(first, stop):
        for s in range(first, stop):
            to_pair[s].wait_recv()

        def body(s, _):
            pq[1, s] = pq[1, s] + drecv[s]
            return 0

        lax.fori_loop(first, stop, body, 0)

    def chunk(k):
        return pl.ds(pl.multiple_of(mod4(k) * 64, 64), 64)

    class Sums:
        def __init__(self, group, first, stop):
            self.group, self.first, self.stop = group, first, stop

        def start(self, step):
            f, t = self.first, self.stop
            self.moved = (
                copies.send(pq.at[1, f:t, 0, chunk(z - 1 - step)], zr.at[step, 0, f:t], up),
                copies.send(pq.at[1, f:t, 1, chunk(z + 1 + step)], zr.at[step, 1, f:t], down),
            )

        def add(self, step):
            f, t = self.first, self.stop
            for d, at in ((0, chunk(z - 2 - step)), (1, chunk(z + 2 + step))):
                self.moved[d].wait_recv()
                pq[1, f:t, d, at] = pq[1, f:t, d, at] + zr[step, d, f:t]

        def advance(self, step):
            self.add(step)
            self.start(step + 1)

        def cross(self):
            self.add(2)
            f, t = self.first, self.stop
            at = pl.ds(pl.multiple_of(z * 64 + (1 - yh) * 32, 32), 32)
            self.crossed = copies.send(pq.at[1, f:t, :, at], yr.at[f:t], far_y)

        def publish(self):
            f, t, g = self.first, self.stop, self.group
            self.crossed.wait_recv()
            at = pl.ds(pl.multiple_of(z * 64 + yh * 32, 32), 32)
            for d in range(2):
                total = pq[1, f:t, d, at] + yr[f:t, d]
                hp[f:t, :, d * quarter : (d + 1) * quarter] = total.astype(BF16)
            me = z * 2 + yh
            self.sent = []
            for n in (0, 3, 1, 2, 4, 5, 6, 7):
                to = (mod4(x + DX[n]), lax.rem(yl + DY[n], 2), x, yl, c)
                copy = pltpu.make_async_remote_copy(
                    src_ref=hp.at[f:t],
                    dst_ref=high.at[f:t, me],
                    send_sem=high_send.at[g, n],
                    recv_sem=high_recv.at[g, me],
                    device_id=to,
                    device_id_type=MESH,
                )
                self.sent.append((n, copy))
                if n == 0:

                    @pl.when(jnp.logical_not(is_self))
                    def _():
                        copy.start()

                    @pl.when(is_self)
                    def _():
                        high[f:t, me] = hp[f:t]
                else:
                    copy.start()

        def arrive(self):
            f, t, g = self.first, self.stop, self.group
            for i in range(8):
                @pl.when(jnp.logical_not(jnp.logical_and(is_self, z * 2 + yh == i)))
                def _():
                    pltpu.make_async_remote_copy(
                        src_ref=hp.at[f:t],
                        dst_ref=high.at[f:t, i],
                        send_sem=high_send.at[g, 0],
                        recv_sem=high_recv.at[g, i],
                        device_id=core,
                        device_id_type=MESH,
                    ).wait_recv()

        def drain(self):
            for n, copy in self.sent:
                if n == 0:
                    pl.when(jnp.logical_not(is_self))(copy.wait_send)
                else:
                    copy.wait_send()

    is_self = jnp.logical_and(z == x, yh == yl)
    a, b, e = Sums(0, 0, 4), Sums(1, 4, 6), Sums(2, 6, 8)

    product(0, 1)
    for copy in late:
        copy.wait()
    cy.wait_recv()
    y_cot = cb(0, 1 - yh, c)
    ycot_up, ycot_down = copies.send(y_cot, y_cot, up), copies.send(y_cot, y_cot, down)
    to_core.append(copies.send(y_cot, y_cot, core))
    cot_half = cot.shape[0] // 2
    ends = []

    def cot_forward(from_down, from_up, y):
        from_down.wait_recv()
        blk = cb(-1, y, c)
        ends.append(copies.send(blk.at[:cot_half], blk.at[:cot_half], up))
        to_core.append(copies.send(blk, blk, core))
        from_up.wait_recv()
        blk = cb(1, y, c)
        ends.append(copies.send(blk.at[cot_half:], blk.at[cot_half:], down))
        to_core.append(copies.send(blk, blk, core))

    cot_forward(cot_up, cot_down, yh)

    hidden.near()
    product(1, 4)
    pair_sum(0, 4)
    a.start(0)
    hidden.far()
    a.advance(0)
    hidden.sides()
    product(4, 6)
    pair_sum(4, 6)
    b.start(0)
    a.advance(1)
    hidden.opposite()
    lowmid = RowGather(copies, lm_all, lm_all.at[0], right, left, across)
    lowmid.own()
    b.advance(0)
    product(6, 7)
    a.cross()
    b.advance(1)
    hidden.last()
    product(7, 8)
    pair_sum(6, 8)
    e.start(0)
    a.publish()
    b.cross()
    e.advance(0)
    cot_forward(ycot_up, ycot_down, 1 - yh)
    b.publish()
    e.advance(1)
    for copy in ends:
        copy.wait_recv()
    for y in (yh, 1 - yh):
        blk = cb(2, y, c)
        to_core.append(copies.send(blk, blk, core))
    e.cross()
    lowmid.near()
    e.publish()
    for copy in to_core:
        copy.wait_recv()
    cot_save = load(cot_all, cot_out)
    lowmid.far()
    lowmid.sides()
    lowmid.opposite()
    lowmid.last()

    def select(row, bx, by):
        rows = dr[pl.ds(row, 256), :]
        lane = lax.broadcasted_iota(jnp.int32, (256, 128), 1)
        for s in range(8):
            base = (mod4(bx + DX[s]) * 2 + lax.rem(by + DY[s], 2)) * 256
            rel = rows - base
            for h in range(2):
                hit = jnp.where(rel == lane + h * 128, 1.0, 0.0).astype(BF16)
                sel[:, s * 256 + h * 128 : s * 256 + (h + 1) * 128] = hit

    wide = lm_all.shape[2]

    def order_lm(i, _):
        row = pl.multiple_of(i * 256, 256)
        select(row, x, yl)
        for h in range(2):
            part = lm_all[:, :, h * depth : (h + 1) * depth].reshape(2048, depth)
            ordered[pl.ds(row, 256), h * depth : (h + 1) * depth] = jnp.dot(
                sel[...], part, preferred_element_type=F32
            ).astype(BF16)
        return 0

    lax.fori_loop(0, 8, order_lm, 0)
    saves = [load(ordered.at[:, 0:wide], ordered_out.at[:, 0:wide])]
    for g in (a, b, e):
        g.arrive()
    for g in (a, b, e):
        g.drain()
    copies.drain()

    ring_at = (mod4(z - 1), mod4(z + 1), mod4(z + 2), z)
    to_pair2 = []

    def join(i):
        base = ring_at[i] * 512

        def order_high(n, _):
            row = pl.multiple_of(base + n * 256, 256)
            select(row, z, yh)
            ordered[pl.ds(row, 256), wide:] = jnp.dot(
                sel[...], high[...].reshape(2048, half), preferred_element_type=F32
            ).astype(BF16)
            return 0

        lax.fori_loop(0, 2, order_high, 0)

        def part(which):
            side = 1 - c if which == 0 else c

            def body(d, _):
                at = pl.multiple_of(base + side * 128, 128)
                rows = jnp.concatenate(
                    [ordered[pl.ds(at, 128), :], ordered[pl.ds(at + 256, 128), :]], axis=0
                )
                value = jnp.dot(rows, wjv[d], preferred_element_type=F32)
                pq[which, 2 * i + d, 0] = value[:, :quarter]
                pq[which, 2 * i + d, 1] = value[:, quarter:]
                return 0

            lax.fori_loop(0, 2, body, 0)

        part(0)
        to_pair2.append(copies.send(pq.at[0, 2 * i : 2 * i + 2], drecv2.at[2 * i : 2 * i + 2], core))
        part(1)

    streams = (1 - yh, yh)
    turns = ((0, 2, 1, 3), (1, 2, 0, 3))

    def both(i, d, st):
        at = pl.ds(pl.multiple_of(streams[st] * 128, 128), 128)
        return pq[1, 2 * i + d, :, at] + drecv2[2 * i + d, :, at]

    moving = {}

    def turn(step, d, st):
        value = both(turns[d][step], d, st)
        if step:
            moving[step - 1, d, st].wait_recv()
            value = value + rb[d, step - 1, st].astype(F32)
        if step < 3:
            sb[d, step, st] = value.astype(BF16)
            to = up if d == 0 else down
            moving[step, d, st] = copies.send(sb.at[d, step, st], rb.at[d, step, st], to)
        return value

    join(0)
    join(1)
    to_pair2[0].wait_recv()
    turn(0, 0, 0)
    turn(0, 0, 1)
    to_pair2[1].wait_recv()
    turn(0, 1, 0)
    turn(0, 1, 1)
    join(2)
    to_pair2[2].wait_recv()
    for st in range(2):
        for d in range(2):
            turn(1, d, st)
    join(3)
    saves.append(load(ordered.at[:, wide:], ordered_out.at[:, wide:]))
    to_pair2[3].wait_recv()
    for st in range(2):
        for d in range(2):
            turn(2, d, st)
    for d in range(2):
        ys[d] = turn(3, d, 0).astype(ys.dtype)
    last = copies.send(ys, yr2, far_y)
    final = [turn(3, d, 1) for d in range(2)]
    last.wait_recv()
    for d in range(2):
        value = (final[d] + yr2[d].astype(F32)).astype(BF16)
        for h in range(2):
            at = d * half + h * quarter
            joined[:, at : at + quarter] = value[h]
    copies.drain()
    cot_save.wait()
    for copy in saves:
        copy.wait()


def on_device(hidden, down_weight, low_feat, mid_feat, draft_rows, join_weight, cotangent):
    tokens = draft_rows.shape[0]
    units, width = down_weight.shape
    depth = low_feat.shape[1]
    half, quarter = width // 2, width // 4
    dr = jnp.broadcast_to(draft_rows[:, None], (tokens, 128))
    anywhere = pl.BlockSpec(memory_space=pl.ANY)
    vmem = pltpu.VMEM
    joined, ordered, cot_all = pl.pallas_call(
        kernel,
        out_shape=(
            jax.ShapeDtypeStruct((128, width), BF16),
            jax.ShapeDtypeStruct((tokens, 3 * depth), BF16),
            jax.ShapeDtypeStruct((16, 128, width), BF16),
        ),
        in_specs=[anywhere] * 7,
        out_specs=(pl.BlockSpec(memory_space=vmem), anywhere, anywhere),
        scratch_shapes=[
            vmem((tokens, 128), jnp.int32),
            vmem((8, 256, units), BF16),
            vmem((4, units, quarter), BF16),
            vmem((8, 256, 2 * depth), BF16),
            vmem((2, 8, 2, 256, quarter), F32),
            vmem((8, 2, 256, quarter), F32),
            vmem((8, 2, 256, quarter), F32),
            vmem((3, 2, 8, 64, quarter), F32),
            vmem((8, 2, 32, quarter), F32),
            vmem((8, 32, half), BF16),
            vmem((8, 8, 32, half), BF16),
            vmem((tokens, 3 * depth), BF16),
            vmem((256, tokens), BF16),
            vmem((2, 3 * depth, half), BF16),
            vmem((2, 3, 2, 2, 128, quarter), BF16),
            vmem((2, 3, 2, 2, 128, quarter), BF16),
            vmem((2, 2, 128, quarter), BF16),
            vmem((2, 2, 128, quarter), BF16),
            vmem((16, 128, width), BF16),
            pltpu.SemaphoreType.DMA((120,)),
            pltpu.SemaphoreType.DMA((120,)),
            pltpu.SemaphoreType.DMA((3, 8)),
            pltpu.SemaphoreType.DMA((3, 8)),
            pltpu.SemaphoreType.DMA((24,)),
        ],
        compiler_params=pltpu.CompilerParams(
            has_side_effects=True, vmem_limit_bytes=66_000_000
        ),
    )(dr, hidden, down_weight, low_feat, mid_feat, join_weight, cotangent)
    grad = lax.dot_general(
        ordered,
        cot_all.reshape(tokens, width),
        (((0,), (0,)), ((), ())),
        preferred_element_type=F32,
    )
    return joined, grad.reshape(3, depth, width)


def solution(mesh):
    finer = Mesh(mesh.devices.reshape(4, 2, 4, 2, 2), AXES)
    in_specs = (
        P(ROWS, TENSOR),
        P(TENSOR, ROWS),
        P(ROWS, TENSOR),
        P(ROWS, TENSOR),
        P(),
        P(None, TENSOR, ROWS),
        P(TENSOR, ROWS),
    )
    out_specs = (P(TENSOR, ROWS), P(None, TENSOR, ROWS))
    return jax.shard_map(
        on_device, mesh=finer, in_specs=in_specs, out_specs=out_specs, check_vma=False
    )
```

```python
import jax
import jax.numpy as jnp
from jax import lax
from jax.experimental import pallas as pl
from jax.experimental.pallas import tpu as pltpu
from jax.sharding import Mesh
from jax.sharding import PartitionSpec as P

AXES = ("x", "yl", "z", "yh", "c")
ROWS = ("x", "yl")
TENSOR = ("z", "yh", "c")
MESH = pl.DeviceIdType.MESH
F32, BF16 = jnp.float32, jnp.bfloat16
DX = (0, 3, 1, 0, 3, 1, 2, 2)
DY = (0, 0, 0, 1, 1, 1, 0, 1)
CUT, MID = 80, 176


def mod4(i):
    return lax.rem(i + 8, 4)


class Copies:
    def __init__(self, send_sems, recv_sems):
        self.send_sems, self.recv_sems, self.made, self.open = send_sems, recv_sems, 0, []

    def send(self, src, dst, to):
        k = self.made
        self.made += 1
        copy = pltpu.make_async_remote_copy(
            src_ref=src,
            dst_ref=dst,
            send_sem=self.send_sems.at[k],
            recv_sem=self.recv_sems.at[k],
            device_id=to,
            device_id_type=MESH,
        )
        copy.start()
        self.open.append(copy)
        return copy

    def drain(self):
        for copy in self.open:
            copy.wait_send()
        self.open = []


class RowGather:
    def __init__(self, copies, buf, src, right, left, across):
        self.send, self.buf, self.src = copies.send, buf, src
        self.right, self.left, self.across = right, left, across

    def own(self):
        b = self.buf
        self.p = self.send(self.src, b.at[3], self.across)
        self.r = self.send(self.src, b.at[1], self.right)
        self.l = self.send(self.src, b.at[2], self.left)

    def near(self):
        b = self.buf
        self.p.wait_recv()
        self.pr = self.send(b.at[3, CUT:], b.at[4, CUT:], self.right)
        self.pl = self.send(b.at[3, CUT:], b.at[5, CUT:], self.left)
        self.r.wait_recv()
        self.fr = self.send(b.at[1, :128], b.at[6, :128], self.right)
        self.yl = self.send(b.at[1, :CUT], b.at[4, :CUT], self.across)
        self.l.wait_recv()
        self.fl = self.send(b.at[2, 128:], b.at[6, 128:], self.left)
        self.yr = self.send(b.at[2, :CUT], b.at[5, :CUT], self.across)

    def far(self):
        b = self.buf
        self.pr.wait_recv()
        self.fpr = self.send(b.at[4, CUT:MID], b.at[7, CUT:MID], self.right)
        self.pl.wait_recv()
        self.fpl = self.send(b.at[5, MID:], b.at[7, MID:], self.left)

    def sides(self):
        self.yl.wait_recv()
        self.yr.wait_recv()

    def opposite(self):
        b = self.buf
        self.fr.wait_recv()
        self.yo = self.send(b.at[6, :CUT], b.at[7, :CUT], self.across)
        self.fl.wait_recv()

    def last(self):
        self.yo.wait_recv()
        self.fpr.wait_recv()
        self.fpl.wait_recv()


def kernel(
    dr_hbm, hid, w, low, mid, wj, cot,
    joined, grad,
    dr, hid_all, w4, lm_all, pq, drecv, drecv2, zr, pr, hp, high, ordered, sel, wjv,
    sb, rb, ys, yr2, cot_all, relay, send_sems, recv_sems, pair_send, pair_recv, over_send,
    over_recv, high_send, high_recv, local, grad_sems,
):
    x, yl, z, yh, c = (lax.axis_index(a) for a in AXES)
    right, left = (mod4(x + 1), yl, z, yh, c), (mod4(x - 1), yl, z, yh, c)
    across = (x, 1 - yl, z, yh, c)
    up, down = (x, yl, mod4(z + 1), yh, c), (x, yl, mod4(z - 1), yh, c)
    far_y, core = (x, yl, z, 1 - yh, c), (x, yl, z, yh, 1 - c)
    between = (x, 1 - yl, z, 1 - yh, c)
    is_self = z == x

    barrier = pltpu.get_barrier_semaphore()
    for to in (right, left, across, between, up, down, far_y, core):
        pl.semaphore_signal(barrier, inc=1, device_id=to, device_id_type=MESH)
    for n in range(4):
        @pl.when(jnp.logical_not(jnp.logical_and(is_self, z == n)))
        def _():
            pl.semaphore_signal(barrier, inc=1, device_id=(z, yl, n, yh, c), device_id_type=MESH)
    pl.semaphore_wait(barrier, jnp.where(is_self, 11, 12))
    copies = Copies(send_sems, recv_sems)
    quarter = w4.shape[2]
    half = 2 * quarter
    nlocal = [0]

    def load(src, dst):
        k = nlocal[0]
        nlocal[0] += 1
        copy = pltpu.make_async_copy(src, dst, local.at[k])
        copy.start()
        return copy

    def cb(dz, y, core_at):
        return cot_all.at[mod4(z + dz) * 4 + y * 2 + core_at]

    own_cot = cb(0, yh, c)
    cot_between = copies.send(cot, relay, between)
    hidden = RowGather(copies, hid_all, hid, right, left, across)
    hidden.own()
    loads = [load(hid, hid_all.at[0])]
    for j in range(4):
        at = pl.multiple_of(lax.rem(c + (1 if j < 2 else 0), 2) * half + (j % 2) * quarter, quarter)
        loads.append(load(w.at[:, pl.ds(at, quarter)], w4.at[j]))
    cot_up, cot_down, to_core = copies.send(cot, own_cot, up), copies.send(cot, own_cot, down), []
    to_core.append(copies.send(cot, own_cot, core))
    late = [load(cot, own_cot), load(low, lm_all.at[0, :, 0 : low.shape[1]])]
    late.append(load(mid, lm_all.at[0, :, low.shape[1] :]))
    late.append(load(dr_hbm, dr))
    depth = low.shape[1]
    for k in range(3):
        for d in range(2):
            late.append(
                load(wj.at[k, :, d * half : (d + 1) * half], wjv.at[d, k * depth : (k + 1) * depth])
            )
    for copy in loads:
        copy.wait()

    def project(first, stop, which):
        def body(i, _):
            s, j = first + i // 2, i % 2
            pq[which, s, j] = jnp.dot(hid_all[s], w4[which * 2 + j], preferred_element_type=F32)
            return 0

        lax.fori_loop(0, 2 * (stop - first), body, 0)

    to_pair = {}

    def product(first, stop):
        project(first, stop, 0)
        for s in range(first, stop):
            to_pair[s] = copies.send(pq.at[0, s], drecv.at[s], core)
        project(first, stop, 1)

    def pair_sum(first, stop):
        for s in range(first, stop):
            to_pair[s].wait_recv()

        def body(s, _):
            pq[1, s] = pq[1, s] + drecv[s]
            return 0

        lax.fori_loop(first, stop, body, 0)

    def chunk(k):
        return pl.ds(pl.multiple_of(mod4(k) * 64, 64), 64)

    class Sums:
        def __init__(self, group, first, stop):
            self.group, self.first, self.stop = group, first, stop

        def start(self, step):
            f, t = self.first, self.stop
            self.moved = (
                copies.send(pq.at[1, f:t, 0, chunk(z - 1 - step)], zr.at[step, 0, f:t], up),
                copies.send(pq.at[1, f:t, 1, chunk(z + 1 + step)], zr.at[step, 1, f:t], down),
            )

        def add(self, step):
            f, t = self.first, self.stop
            for d, at in ((0, chunk(z - 2 - step)), (1, chunk(z + 2 + step))):
                self.moved[d].wait_recv()
                pq[1, f:t, d, at] = pq[1, f:t, d, at] + zr[step, d, f:t]

        def advance(self, step):
            self.add(step)
            self.start(step + 1)

        def cross(self):
            self.add(2)
            f, t, g = self.first, self.stop, self.group
            self.pair = pltpu.make_async_remote_copy(
                src_ref=pq.at[1, f:t, :, chunk(z)],
                dst_ref=pr.at[yh, f:t],
                send_sem=pair_send.at[g],
                recv_sem=pair_recv.at[g, yh],
                device_id=(x, 1 - yl, z, yl, c),
                device_id_type=MESH,
            )
            self.pair.start()
            self.over = pltpu.make_async_remote_copy(
                src_ref=hp.at[f:t],
                dst_ref=hp.at[f:t],
                send_sem=over_send.at[g],
                recv_sem=over_recv.at[g],
                device_id=across,
                device_id_type=MESH,
            )

        def readers(self):
            f, t, g = self.first, self.stop, self.group
            made = []
            for n in range(4):
                made.append(
                    pltpu.make_async_remote_copy(
                        src_ref=hp.at[f:t],
                        dst_ref=high.at[f:t, z],
                        send_sem=high_send.at[g, n],
                        recv_sem=high_recv.at[g, z],
                        device_id=(mod4(x + n), yl, x, yh, c),
                        device_id_type=MESH,
                    )
                )
            return made

        def publish(self):
            f, t = self.first, self.stop
            made = self.readers()
            for n in (2, 1, 3):
                made[n].start()
            pl.when(jnp.logical_not(is_self))(made[0].start)

            @pl.when(is_self)
            def _():
                high[f:t, z] = hp[f:t]

        def total(self):
            f, t, g = self.first, self.stop, self.group

            @pl.when(yh != yl)
            def _():
                for n in range(2):
                    pltpu.make_async_remote_copy(
                        src_ref=pr.at[n, f:t],
                        dst_ref=pr.at[n, f:t],
                        send_sem=pair_send.at[g],
                        recv_sem=pair_recv.at[g, n],
                        device_id=across,
                        device_id_type=MESH,
                    ).wait_recv()
                for d in range(2):
                    value = pr[0, f:t, d] + pr[1, f:t, d]
                    hp[f:t, :, d * quarter : (d + 1) * quarter] = value.astype(BF16)
                self.over.start()
                self.publish()

        def follow(self):
            @pl.when(yh == yl)
            def _():
                self.over.wait_recv()
                self.publish()

        def arrive(self):
            f, t, g = self.first, self.stop, self.group
            for i in range(4):
                @pl.when(jnp.logical_not(jnp.logical_and(is_self, z == i)))
                def _():
                    pltpu.make_async_remote_copy(
                        src_ref=hp.at[f:t],
                        dst_ref=high.at[f:t, i],
                        send_sem=high_send.at[g, 0],
                        recv_sem=high_recv.at[g, i],
                        device_id=core,
                        device_id_type=MESH,
                    ).wait_recv()

        def drain(self):
            self.pair.wait_send()
            pl.when(yh != yl)(self.over.wait_send)
            made = self.readers()
            for n in (2, 1, 3):
                made[n].wait_send()
            pl.when(jnp.logical_not(is_self))(made[0].wait_send)

    a, b, e = Sums(0, 0, 4), Sums(1, 4, 6), Sums(2, 6, 8)

    product(0, 1)
    for copy in late:
        copy.wait()
    cot_half = cot.shape[0] // 2
    ends = []

    def cot_forward(from_down, from_up, y):
        from_down.wait_recv()
        blk = cb(-1, y, c)
        ends.append(copies.send(blk.at[:cot_half], blk.at[:cot_half], up))
        to_core.append(copies.send(blk, blk, core))
        from_up.wait_recv()
        blk = cb(1, y, c)
        ends.append(copies.send(blk.at[cot_half:], blk.at[cot_half:], down))
        to_core.append(copies.send(blk, blk, core))

    y_cot = cb(0, 1 - yh, c)
    cot_between.wait_recv()
    cot_over = copies.send(relay, y_cot, across)
    cot_forward(cot_up, cot_down, yh)

    hidden.near()
    product(1, 4)
    pair_sum(0, 4)
    a.start(0)
    cot_over.wait_recv()
    ycot_up, ycot_down = copies.send(y_cot, y_cot, up), copies.send(y_cot, y_cot, down)
    to_core.append(copies.send(y_cot, y_cot, core))
    hidden.far()
    lowmid = RowGather(copies, lm_all, lm_all.at[0], right, left, across)
    lowmid.own()
    a.advance(0)
    hidden.sides()
    product(4, 6)
    pair_sum(4, 6)
    b.start(0)
    a.advance(1)
    hidden.opposite()
    product(6, 7)
    b.advance(0)
    a.cross()
    b.advance(1)
    hidden.last()
    product(7, 8)
    pair_sum(6, 8)
    e.start(0)
    b.cross()
    e.advance(0)
    lowmid.near()
    a.total()
    e.advance(1)
    lowmid.far()
    b.total()
    a.follow()
    e.cross()
    lowmid.sides()
    lowmid.opposite()
    b.follow()
    e.total()
    lowmid.last()
    e.follow()
    cot_forward(ycot_up, ycot_down, 1 - yh)
    for copy in ends:
        copy.wait_recv()
    for y in (yh, 1 - yh):
        blk = cb(2, y, c)
        to_core.append(copies.send(blk, blk, core))

    def select(row, bx, by):
        rows = dr[pl.ds(row, 256), :]
        lane = lax.broadcasted_iota(jnp.int32, (256, 128), 1)
        for s in range(8):
            base = (mod4(bx + DX[s]) * 2 + lax.rem(by + DY[s], 2)) * 256
            rel = rows - base
            for h in range(2):
                hit = jnp.where(rel == lane + h * 128, 1.0, 0.0).astype(BF16)
                sel[:, s * 256 + h * 128 : s * 256 + (h + 1) * 128] = hit

    wide = lm_all.shape[2]

    def order_lm(i, _):
        row = pl.multiple_of(i * 256, 256)
        select(row, x, yl)
        for h in range(2):
            part = lm_all[:, :, h * depth : (h + 1) * depth].reshape(2048, depth)
            ordered[pl.ds(row, 256), h * depth : (h + 1) * depth] = jnp.dot(
                sel[...], part, preferred_element_type=F32
            ).astype(BF16)
        return 0

    lax.fori_loop(0, 8, order_lm, 0)
    for copy in to_core:
        copy.wait_recv()

    def saving(n, slot, part):
        row = pl.multiple_of(lax.rem(n, depth // 256) * 256, 256)
        return pltpu.make_async_copy(
            drecv.at[slot * 2 + part // 2, part % 2],
            grad.at[n // (depth // 256), pl.ds(row, 256), part * quarter : (part + 1) * quarter],
            grad_sems.at[n, part],
        )

    def gradient(first, stop):
        def body(n, _):
            slot = lax.rem(n, 4)
            features = ordered[:, pl.ds(pl.multiple_of(n * 256, 256), 256)]
            value = lax.dot_general(
                features,
                cot_all[...].reshape(features.shape[0], 2 * half),
                (((0,), (0,)), ((), ())),
                preferred_element_type=F32,
            )
            for part in range(4):
                at = part * quarter
                drecv[slot * 2 + part // 2, part % 2] = value[:, at : at + quarter]
            for part in range(4):
                saving(n, slot, part).start()
            return 0

        lax.fori_loop(first, stop, body, 0)

    def saved(first, stop):
        for n in range(first, stop):
            for part in range(4):
                saving(n, n % 4, part).wait()

    gradient(0, 4)
    for g in (a, b, e):
        g.arrive()
    for g in (a, b, e):
        g.drain()
    copies.drain()

    ring_at = (mod4(z - 1), mod4(z + 1), mod4(z + 2), z)
    to_pair2 = []

    def join(i):
        base = ring_at[i] * 512

        def order_high(n, _):
            row = pl.multiple_of(base + n * 256, 256)
            select(row, z, yh)
            ordered[pl.ds(row, 256), wide:] = jnp.dot(
                sel[...], high[...].reshape(2048, half), preferred_element_type=F32
            ).astype(BF16)
            return 0

        lax.fori_loop(0, 2, order_high, 0)

        def part(which):
            side = 1 - c if which == 0 else c

            def body(d, _):
                at = pl.multiple_of(base + side * 128, 128)
                rows = jnp.concatenate(
                    [ordered[pl.ds(at, 128), :], ordered[pl.ds(at + 256, 128), :]], axis=0
                )
                value = jnp.dot(rows, wjv[d], preferred_element_type=F32)
                pq[which, 2 * i + d, 0] = value[:, :quarter]
                pq[which, 2 * i + d, 1] = value[:, quarter:]
                return 0

            lax.fori_loop(0, 2, body, 0)

        part(0)
        to_pair2.append(copies.send(pq.at[0, 2 * i : 2 * i + 2], drecv2.at[2 * i : 2 * i + 2], core))
        part(1)

    streams = (1 - yh, yh)
    turns = ((0, 2, 1, 3), (1, 2, 0, 3))

    def both(i, d, st):
        at = pl.ds(pl.multiple_of(streams[st] * 128, 128), 128)
        return pq[1, 2 * i + d, :, at] + drecv2[2 * i + d, :, at]

    moving = {}

    def turn(step, d, st):
        value = both(turns[d][step], d, st)
        if step:
            moving[step - 1, d, st].wait_recv()
            value = value + rb[d, step - 1, st].astype(F32)
        if step < 3:
            sb[d, step, st] = value.astype(BF16)
            to = up if d == 0 else down
            moving[step, d, st] = copies.send(sb.at[d, step, st], rb.at[d, step, st], to)
        return value

    join(0)
    join(1)
    to_pair2[0].wait_recv()
    turn(0, 0, 0)
    turn(0, 0, 1)
    to_pair2[1].wait_recv()
    turn(0, 1, 0)
    turn(0, 1, 1)
    join(2)
    to_pair2[2].wait_recv()
    for st in range(2):
        for d in range(2):
            turn(1, d, st)
    join(3)
    to_pair2[3].wait_recv()
    for st in range(2):
        for d in range(2):
            turn(2, d, st)
    saved(0, 2)
    gradient(4, 6)
    for d in range(2):
        ys[d] = turn(3, d, 0).astype(ys.dtype)
    last = copies.send(ys, yr2, far_y)
    final = [turn(3, d, 1) for d in range(2)]
    last.wait_recv()
    for d in range(2):
        value = (final[d] + yr2[d].astype(F32)).astype(BF16)
        for h in range(2):
            at = d * half + h * quarter
            joined[:, at : at + quarter] = value[h]
    copies.drain()
    saved(2, 6)


def on_device(hidden, down_weight, low_feat, mid_feat, draft_rows, join_weight, cotangent):
    tokens = draft_rows.shape[0]
    units, width = down_weight.shape
    depth = low_feat.shape[1]
    half, quarter = width // 2, width // 4
    dr = jnp.broadcast_to(draft_rows[:, None], (tokens, 128))
    anywhere = pl.BlockSpec(memory_space=pl.ANY)
    vmem = pltpu.VMEM
    joined, grad = pl.pallas_call(
        kernel,
        out_shape=(
            jax.ShapeDtypeStruct((128, width), BF16),
            jax.ShapeDtypeStruct((3, depth, width), F32),
        ),
        in_specs=[anywhere] * 7,
        out_specs=(pl.BlockSpec(memory_space=vmem), anywhere),
        scratch_shapes=[
            vmem((tokens, 128), jnp.int32),
            vmem((8, 256, units), BF16),
            vmem((4, units, quarter), BF16),
            vmem((8, 256, 2 * depth), BF16),
            vmem((2, 8, 2, 256, quarter), F32),
            vmem((8, 2, 256, quarter), F32),
            vmem((8, 2, 256, quarter), F32),
            vmem((3, 2, 8, 64, quarter), F32),
            vmem((2, 8, 2, 64, quarter), F32),
            vmem((8, 64, half), BF16),
            vmem((8, 4, 64, half), BF16),
            vmem((tokens, 3 * depth), BF16),
            vmem((256, tokens), BF16),
            vmem((2, 3 * depth, half), BF16),
            vmem((2, 3, 2, 2, 128, quarter), BF16),
            vmem((2, 3, 2, 2, 128, quarter), BF16),
            vmem((2, 2, 128, quarter), BF16),
            vmem((2, 2, 128, quarter), BF16),
            vmem((16, 128, width), BF16),
            vmem((128, width), BF16),
            pltpu.SemaphoreType.DMA((120,)),
            pltpu.SemaphoreType.DMA((120,)),
            pltpu.SemaphoreType.DMA((3,)),
            pltpu.SemaphoreType.DMA((3, 2)),
            pltpu.SemaphoreType.DMA((3,)),
            pltpu.SemaphoreType.DMA((3,)),
            pltpu.SemaphoreType.DMA((3, 4)),
            pltpu.SemaphoreType.DMA((3, 4)),
            pltpu.SemaphoreType.DMA((24,)),
            pltpu.SemaphoreType.DMA((6, 4)),
        ],
        compiler_params=pltpu.CompilerParams(
            collective_id=0, has_side_effects=True, vmem_limit_bytes=66_000_000
        ),
    )(dr, hidden, down_weight, low_feat, mid_feat, join_weight, cotangent)
    return joined, grad


def solution(mesh):
    finer = Mesh(mesh.devices.reshape(4, 2, 4, 2, 2), AXES)
    in_specs = (
        P(ROWS, TENSOR),
        P(TENSOR, ROWS),
        P(ROWS, TENSOR),
        P(ROWS, TENSOR),
        P(),
        P(None, TENSOR, ROWS),
        P(TENSOR, ROWS),
    )
    out_specs = (P(TENSOR, ROWS), P(None, TENSOR, ROWS))
    return jax.shard_map(
        on_device, mesh=finer, in_specs=in_specs, out_specs=out_specs, check_vma=False
    )
```

```python
import jax
import jax.numpy as jnp
from jax import lax
from jax.experimental import pallas as pl
from jax.experimental.pallas import tpu as pltpu
from jax.sharding import Mesh
from jax.sharding import PartitionSpec as P

AXES = ("x", "yl", "z", "yh", "c")
ROWS = ("x", "yl")
TENSOR = ("z", "yh", "c")
MESH = pl.DeviceIdType.MESH
F32, BF16 = jnp.float32, jnp.bfloat16
DX = (0, 3, 1, 0, 3, 1, 2, 2)
DY = (0, 0, 0, 1, 1, 1, 0, 1)
CUT, MID = 96, 176


def mod4(i):
    return lax.rem(i + 8, 4)


class Copies:
    def __init__(self, send_sems, recv_sems):
        self.send_sems, self.recv_sems, self.made, self.open = send_sems, recv_sems, 0, []

    def send(self, src, dst, to):
        k = self.made
        self.made += 1
        copy = pltpu.make_async_remote_copy(
            src_ref=src,
            dst_ref=dst,
            send_sem=self.send_sems.at[k],
            recv_sem=self.recv_sems.at[k],
            device_id=to,
            device_id_type=MESH,
        )
        copy.start()
        self.open.append(copy)
        return copy

    def drain(self):
        for copy in self.open:
            copy.wait_send()
        self.open = []


class RowGather:
    def __init__(self, copies, buf, src, right, left, across):
        self.send, self.buf, self.src = copies.send, buf, src
        self.right, self.left, self.across = right, left, across

    def own(self):
        b = self.buf
        self.p = self.send(self.src, b.at[3], self.across)
        self.r = self.send(self.src, b.at[1], self.right)
        self.l = self.send(self.src, b.at[2], self.left)

    def near(self):
        b = self.buf
        self.p.wait_recv()
        self.pr = self.send(b.at[3, CUT:], b.at[4, CUT:], self.right)
        self.pl = self.send(b.at[3, CUT:], b.at[5, CUT:], self.left)
        self.r.wait_recv()
        self.fr = self.send(b.at[1, :128], b.at[6, :128], self.right)
        self.yl = self.send(b.at[1, :CUT], b.at[4, :CUT], self.across)
        self.l.wait_recv()
        self.fl = self.send(b.at[2, 128:], b.at[6, 128:], self.left)
        self.yr = self.send(b.at[2, :CUT], b.at[5, :CUT], self.across)

    def far(self):
        b = self.buf
        self.pr.wait_recv()
        self.fpr = self.send(b.at[4, CUT:MID], b.at[7, CUT:MID], self.right)
        self.pl.wait_recv()
        self.fpl = self.send(b.at[5, MID:], b.at[7, MID:], self.left)

    def sides(self):
        self.yl.wait_recv()
        self.yr.wait_recv()

    def opposite(self):
        b = self.buf
        self.fr.wait_recv()
        self.yo = self.send(b.at[6, :CUT], b.at[7, :CUT], self.across)
        self.fl.wait_recv()

    def last(self):
        self.yo.wait_recv()
        self.fpr.wait_recv()
        self.fpl.wait_recv()


def kernel(
    rows_hbm, hid, w, low, mid, wj, cot,
    joined, grad,
    rows_in, dr, hid_all, w4, lm_all, pq, drecv, drecv2, zr, pr, hp, hx, high, ordered, sel, wjv,
    sb, rb, ys, yr2, cot_all, relay, send_sems, recv_sems, pair_send, pair_recv, over_send,
    over_recv, ring_send, ring_recv, high_send, high_recv, swap_send, swap_recv, local, grad_sems,
):
    x, yl, z, yh, c = (lax.axis_index(a) for a in AXES)
    right, left = (mod4(x + 1), yl, z, yh, c), (mod4(x - 1), yl, z, yh, c)
    across = (x, 1 - yl, z, yh, c)
    up, down = (x, yl, mod4(z + 1), yh, c), (x, yl, mod4(z - 1), yh, c)
    far_y, core = (x, yl, z, 1 - yh, c), (x, yl, z, yh, 1 - c)
    between = (x, 1 - yl, z, 1 - yh, c)
    far_z = (x, yl, mod4(z + 2), yh, c)

    barrier = pltpu.get_barrier_semaphore()
    partners = (right, left, across, between, up, down, far_z, far_y, core)
    for to in partners:
        pl.semaphore_signal(barrier, inc=1, device_id=to, device_id_type=MESH)
    pl.semaphore_wait(barrier, len(partners))
    copies = Copies(send_sems, recv_sems)
    quarter = w4.shape[2]
    half = 2 * quarter
    nlocal = [0]

    def load(src, dst):
        k = nlocal[0]
        nlocal[0] += 1
        copy = pltpu.make_async_copy(src, dst, local.at[k])
        copy.start()
        return copy

    def cb(dz, y, core_at):
        return cot_all.at[mod4(z + dz) * 4 + y * 2 + core_at]

    own_cot = cb(0, yh, c)
    cot_between = copies.send(cot, relay, between)
    hidden = RowGather(copies, hid_all, hid, right, left, across)
    hidden.own()
    loads = [load(hid, hid_all.at[0])]
    for j in range(4):
        at = pl.multiple_of(lax.rem(c + (1 if j < 2 else 0), 2) * half + (j % 2) * quarter, quarter)
        loads.append(load(w.at[:, pl.ds(at, quarter)], w4.at[j]))
    cot_up, cot_down, to_core = copies.send(cot, own_cot, up), copies.send(cot, own_cot, down), []
    to_core.append(copies.send(cot, own_cot, core))
    late = [load(cot, own_cot), load(low, lm_all.at[0, :, 0 : low.shape[1]])]
    late.append(load(mid, lm_all.at[0, :, low.shape[1] :]))
    late.append(load(rows_hbm, rows_in))
    depth = low.shape[1]
    for k in range(3):
        for d in range(2):
            late.append(
                load(wj.at[k, :, d * half : (d + 1) * half], wjv.at[d, k * depth : (k + 1) * depth])
            )
    for copy in loads:
        copy.wait()

    def project(first, stop, which):
        def body(i, _):
            s, j = first + i // 2, i % 2
            pq[which, s, j] = jnp.dot(hid_all[s], w4[which * 2 + j], preferred_element_type=F32)
            return 0

        lax.fori_loop(0, 2 * (stop - first), body, 0)

    to_pair = {}

    def product(first, stop):
        project(first, stop, 0)
        for s in range(first, stop):
            to_pair[s] = copies.send(pq.at[0, s], drecv.at[s], core)
        project(first, stop, 1)

    def pair_sum(first, stop):
        for s in range(first, stop):
            to_pair[s].wait_recv()

        def body(s, _):
            pq[1, s] = pq[1, s] + drecv[s]
            return 0

        lax.fori_loop(first, stop, body, 0)

    def chunk(k):
        return pl.ds(pl.multiple_of(mod4(k) * 64, 64), 64)

    class Sums:
        def __init__(self, group, first, stop):
            self.group, self.first, self.stop = group, first, stop

        def start(self, step):
            f, t = self.first, self.stop
            self.moved = (
                copies.send(pq.at[1, f:t, 0, chunk(z - 1 - step)], zr.at[step, 0, f:t], up),
                copies.send(pq.at[1, f:t, 1, chunk(z + 1 + step)], zr.at[step, 1, f:t], down),
            )

        def add(self, step):
            f, t = self.first, self.stop
            for d, at in ((0, chunk(z - 2 - step)), (1, chunk(z + 2 + step))):
                self.moved[d].wait_recv()
                pq[1, f:t, d, at] = pq[1, f:t, d, at] + zr[step, d, f:t]

        def advance(self, step):
            self.add(step)
            self.start(step + 1)

        def cross(self):
            self.add(2)
            f, t, g = self.first, self.stop, self.group
            self.pair = pltpu.make_async_remote_copy(
                src_ref=pq.at[1, f:t, :, chunk(z)],
                dst_ref=pr.at[yh, f:t],
                send_sem=pair_send.at[g],
                recv_sem=pair_recv.at[g, yh],
                device_id=(x, 1 - yl, z, yl, c),
                device_id_type=MESH,
            )
            self.pair.start()
            self.over = pltpu.make_async_remote_copy(
                src_ref=hp.at[f:t],
                dst_ref=hp.at[f:t],
                send_sem=over_send.at[g],
                recv_sem=over_recv.at[g],
                device_id=across,
                device_id_type=MESH,
            )

        def total(self):
            f, t, g = self.first, self.stop, self.group

            @pl.when(yh != yl)
            def _():
                for n in range(2):
                    pltpu.make_async_remote_copy(
                        src_ref=pr.at[n, f:t],
                        dst_ref=pr.at[n, f:t],
                        send_sem=pair_send.at[g],
                        recv_sem=pair_recv.at[g, n],
                        device_id=across,
                        device_id_type=MESH,
                    ).wait_recv()
                for d in range(2):
                    value = pr[0, f:t, d] + pr[1, f:t, d]
                    hp[f:t, :, d * quarter : (d + 1) * quarter] = value.astype(BF16)
                self.over.start()

        def to_reader(self, n):
            f, t, g = self.first, self.stop, self.group
            src = hp if n == 0 else hx.at[n - 1]
            at = mod4(x + (0, 3, 1, 2)[n])
            copy = pltpu.make_async_remote_copy(
                src_ref=src.at[f:t],
                dst_ref=high.at[f:t, z],
                send_sem=high_send.at[g, n],
                recv_sem=high_recv.at[g, z],
                device_id=(x, yl, at, yh, c),
                device_id_type=MESH,
            )
            return copy, at, src

        def read(self, n):
            f, t = self.first, self.stop
            copy, at, src = self.to_reader(n)
            pl.when(at != z)(copy.start)

            @pl.when(at == z)
            def _():
                high[f:t, z] = src[f:t]

        def ring(self, n, src, dst, to):
            copy = pltpu.make_async_remote_copy(
                src_ref=src,
                dst_ref=dst,
                send_sem=ring_send.at[self.group, n],
                recv_sem=ring_recv.at[self.group, n],
                device_id=to,
                device_id_type=MESH,
            )
            copy.start()
            self.rings.append(copy)

        def publish(self):
            f, t = self.first, self.stop

            @pl.when(yh == yl)
            def _():
                self.over.wait_recv()

            self.rings = []
            self.ring(0, hp.at[f:t], hx.at[0, f:t], right)
            self.ring(1, hp.at[f:t], hx.at[1, f:t], left)
            self.read(0)

        def forward(self):
            f, t = self.first, self.stop
            self.rings[0].wait_recv()
            self.ring(2, hx.at[0, f:t, :32], hx.at[2, f:t, :32], right)
            self.read(1)
            self.rings[1].wait_recv()
            self.ring(3, hx.at[1, f:t, 32:], hx.at[2, f:t, 32:], left)
            self.read(2)

        def finish(self):
            self.rings[2].wait_recv()
            self.rings[3].wait_recv()
            self.read(3)

        def arrive(self):
            f, t, g = self.first, self.stop, self.group
            for i in range(4):
                @pl.when(z != i)
                def _():
                    pltpu.make_async_remote_copy(
                        src_ref=hp.at[f:t],
                        dst_ref=high.at[f:t, i],
                        send_sem=high_send.at[g, 0],
                        recv_sem=high_recv.at[g, i],
                        device_id=core,
                        device_id_type=MESH,
                    ).wait_recv()

        def drain(self):
            self.pair.wait_send()
            pl.when(yh != yl)(self.over.wait_send)
            for copy in self.rings:
                copy.wait_send()
            for n in range(4):
                copy, at, _ = self.to_reader(n)
                pl.when(at != z)(copy.wait_send)

    a, b, e, f = Sums(0, 0, 4), Sums(1, 4, 6), Sums(2, 6, 7), Sums(3, 7, 8)
    groups = (a, b, e, f)

    product(0, 1)
    for copy in late:
        copy.wait()
    cot_half = cot.shape[0] // 2
    ends = []

    def cot_forward(from_down, from_up, y):
        from_down.wait_recv()
        blk = cb(-1, y, c)
        ends.append(copies.send(blk.at[:cot_half], blk.at[:cot_half], up))
        to_core.append(copies.send(blk, blk, core))
        from_up.wait_recv()
        blk = cb(1, y, c)
        ends.append(copies.send(blk.at[cot_half:], blk.at[cot_half:], down))
        to_core.append(copies.send(blk, blk, core))

    for i in range(16):
        lanes = jnp.broadcast_to(rows_in[i : i + 1, :], (128, 128)).astype(F32)
        dr[i * 128 : (i + 1) * 128, :] = lanes.T.astype(jnp.int32)

    def select(row, bx, by):
        rows = dr[pl.ds(row, 256), :]
        lane = lax.broadcasted_iota(jnp.int32, (256, 128), 1)
        for s in range(8):
            base = (mod4(bx + DX[s]) * 2 + lax.rem(by + DY[s], 2)) * 256
            rel = rows - base
            for h in range(2):
                hit = jnp.where(rel == lane + h * 128, 1.0, 0.0).astype(BF16)
                sel[:, s * 256 + h * 128 : s * 256 + (h + 1) * 128] = hit

    wide = lm_all.shape[2]

    def order_lm(first, stop):
        def body(i, _):
            row = pl.multiple_of(i * 256, 256)
            select(row, x, yl)

            def columns(h, _):
                at = pl.ds(pl.multiple_of(h * depth, depth), depth)
                ordered[pl.ds(row, 256), at] = jnp.dot(
                    sel[...], lm_all[:, :, at].reshape(2048, depth), preferred_element_type=F32
                ).astype(BF16)
                return 0

            lax.fori_loop(0, 2, columns, 0)
            return 0

        lax.fori_loop(first, stop, body, 0)

    y_cot = cb(0, 1 - yh, c)
    cot_between.wait_recv()
    cot_forward(cot_up, cot_down, yh)

    hidden.near()
    product(1, 4)
    pair_sum(0, 4)
    a.start(0)
    hidden.far()
    lowmid = RowGather(copies, lm_all, lm_all.at[0], right, left, across)
    lowmid.own()
    a.advance(0)
    hidden.sides()
    product(4, 6)
    hidden.opposite()
    cot_over = copies.send(relay, y_cot, across)
    pair_sum(4, 6)
    b.start(0)
    a.advance(1)
    product(6, 7)
    b.advance(0)
    pair_sum(6, 7)
    e.start(0)
    a.cross()
    b.advance(1)
    e.advance(0)
    hidden.last()
    product(7, 8)
    b.cross()
    pair_sum(7, 8)
    f.start(0)
    e.advance(1)
    lowmid.near()
    f.advance(0)
    e.cross()
    cot_over.wait_recv()
    ycot_up, ycot_down = copies.send(y_cot, y_cot, up), copies.send(y_cot, y_cot, down)
    to_core.append(copies.send(y_cot, y_cot, core))
    lowmid.far()
    f.advance(1)
    a.total()
    lowmid.opposite()
    f.cross()
    b.total()
    a.publish()
    e.total()
    b.publish()
    f.total()
    e.publish()
    cot_forward(ycot_up, ycot_down, 1 - yh)
    a.forward()
    f.publish()
    lowmid.sides()
    lowmid.last()
    order_lm(0, 2)
    b.forward()
    a.finish()
    e.forward()
    order_lm(2, 4)
    f.forward()
    b.finish()
    e.finish()
    f.finish()
    order_lm(4, 8)
    for copy in ends:
        copy.wait_recv()
    for y in (yh, 1 - yh):
        blk = cb(2, y, c)
        to_core.append(copies.send(blk, blk, core))
    for copy in to_core:
        copy.wait_recv()

    def saving(n, slot, part):
        row = pl.multiple_of(lax.rem(n, depth // 256) * 256, 256)
        return pltpu.make_async_copy(
            drecv.at[slot * 2 + part // 2, part % 2],
            grad.at[n // (depth // 256), pl.ds(row, 256), part * quarter : (part + 1) * quarter],
            grad_sems.at[n, part],
        )

    def gradient(first, stop):
        def body(n, _):
            slot = lax.rem(n, 4)
            features = ordered[:, pl.ds(pl.multiple_of(n * 256, 256), 256)]
            value = lax.dot_general(
                features,
                cot_all[...].reshape(features.shape[0], 2 * half),
                (((0,), (0,)), ((), ())),
                preferred_element_type=F32,
            )
            for part in range(4):
                at = part * quarter
                drecv[slot * 2 + part // 2, part % 2] = value[:, at : at + quarter]
            for part in range(4):
                saving(n, slot, part).start()
            return 0

        lax.fori_loop(first, stop, body, 0)

    def saved(first, stop):
        for n in range(first, stop):
            for part in range(4):
                saving(n, n % 4, part).wait()

    gradient(0, 2)
    for g in groups:
        g.arrive()
    for g in groups:
        g.drain()
    copies.drain()

    ring_at = (mod4(z - 1), mod4(z + 1), mod4(z + 2), z)

    def order_high(i):
        def body(n, _):
            row = pl.multiple_of(ring_at[i] * 512 + n * 256, 256)
            select(row, z, yh)
            ordered[pl.ds(row, 256), wide:] = jnp.dot(
                sel[...], high[...].reshape(2048, half), preferred_element_type=F32
            ).astype(BF16)
            return 0

        lax.fori_loop(0, 2, body, 0)

    paired = {}

    def join(i, d):
        def part(which, _):
            side = lax.rem(c + 1 - which, 2)
            at = pl.multiple_of(ring_at[i] * 512 + side * 128, 128)
            rows = jnp.concatenate(
                [ordered[pl.ds(at, 128), :], ordered[pl.ds(at + 256, 128), :]], axis=0
            )
            value = jnp.dot(rows, wjv[d], preferred_element_type=F32)
            pq[which, 2 * i + d, 0] = value[:, :quarter]
            pq[which, 2 * i + d, 1] = value[:, quarter:]

            @pl.when(which == 0)
            def _():
                swap(i, d).start()

            return 0

        lax.fori_loop(0, 2, part, 0)
        paired[i, d] = swap(i, d)

    def swap(i, d):
        return pltpu.make_async_remote_copy(
            src_ref=pq.at[0, 2 * i + d],
            dst_ref=drecv2.at[2 * i + d],
            send_sem=swap_send.at[i, d],
            recv_sem=swap_recv.at[i, d],
            device_id=core,
            device_id_type=MESH,
        )

    streams = (1 - yh, yh)
    turns = ((0, 2, 1, 3), (1, 2, 0, 3))

    def both(i, d, st):
        at = pl.ds(pl.multiple_of(streams[st] * 128, 128), 128)
        return pq[1, 2 * i + d, :, at] + drecv2[2 * i + d, :, at]

    moving = {}

    def turn(step, d, st):
        value = both(turns[d][step], d, st)
        if step:
            moving[step - 1, d, st].wait_recv()
            value = value + rb[d, step - 1, st].astype(F32)
        if step < 3:
            sb[d, step, st] = value.astype(BF16)
            to = up if d == 0 else down
            moving[step, d, st] = copies.send(sb.at[d, step, st], rb.at[d, step, st], to)
        return value

    order_high(0)
    join(0, 0)
    order_high(1)
    join(1, 1)
    paired[0, 0].wait_recv()
    turn(0, 0, 0)
    turn(0, 0, 1)
    paired[1, 1].wait_recv()
    turn(0, 1, 0)
    turn(0, 1, 1)
    order_high(2)
    join(2, 0)
    join(2, 1)
    join(1, 0)
    paired[2, 0].wait_recv()
    paired[2, 1].wait_recv()
    for st in range(2):
        for d in range(2):
            turn(1, d, st)
    join(0, 1)
    order_high(3)
    join(3, 0)
    join(3, 1)
    paired[1, 0].wait_recv()
    paired[0, 1].wait_recv()
    for st in range(2):
        for d in range(2):
            turn(2, d, st)
    gradient(2, 4)
    paired[3, 0].wait_recv()
    paired[3, 1].wait_recv()
    for d in range(2):
        ys[d] = turn(3, d, 0).astype(ys.dtype)
    last = copies.send(ys, yr2, far_y)
    final = [turn(3, d, 1) for d in range(2)]
    saved(0, 2)
    gradient(4, 6)
    last.wait_recv()
    for d in range(2):
        value = (final[d] + yr2[d].astype(F32)).astype(BF16)
        for h in range(2):
            at = d * half + h * quarter
            joined[:, at : at + quarter] = value[h]
    copies.drain()
    for copy in paired.values():
        copy.wait_send()
    saved(2, 6)


def deliver(joined, grad, joined_out, grad_out, joined_buf, grad_buf, sems):
    blocks = [(joined, joined_buf, joined_out)]
    rows = grad.shape[1] // 2
    for k in range(3):
        for h in range(2):
            at = (k, pl.ds(h * rows, rows))
            blocks.append((grad.at[at], grad_buf.at[at], grad_out.at[at]))
    loads = [pltpu.make_async_copy(s, b, sems.at[0, n]) for n, (s, b, _) in enumerate(blocks)]
    stores = [pltpu.make_async_copy(b, o, sems.at[1, n]) for n, (_, b, o) in enumerate(blocks)]
    for copy in loads:
        copy.start()
    for copy, store in zip(loads, stores):
        copy.wait()
        store.start()
    for store in stores:
        store.wait()


def on_device(hidden, down_weight, low_feat, mid_feat, draft_rows, join_weight, cotangent):
    tokens = draft_rows.shape[0]
    units, width = down_weight.shape
    depth = low_feat.shape[1]
    half, quarter = width // 2, width // 4
    rows = draft_rows.reshape(tokens // 128, 128)
    anywhere = pl.BlockSpec(memory_space=pl.ANY)
    vmem = pltpu.VMEM
    joined, grad = pl.pallas_call(
        kernel,
        out_shape=(
            jax.ShapeDtypeStruct((128, width), BF16),
            jax.ShapeDtypeStruct((3, depth, width), F32),
        ),
        in_specs=[anywhere] * 7,
        out_specs=(pl.BlockSpec(memory_space=vmem), anywhere),
        scratch_shapes=[
            vmem((tokens // 128, 128), jnp.int32),
            vmem((tokens, 128), jnp.int32),
            vmem((8, 256, units), BF16),
            vmem((4, units, quarter), BF16),
            vmem((8, 256, 2 * depth), BF16),
            vmem((2, 8, 2, 256, quarter), F32),
            vmem((8, 2, 256, quarter), F32),
            vmem((8, 2, 256, quarter), F32),
            vmem((3, 2, 8, 64, quarter), F32),
            vmem((2, 8, 2, 64, quarter), F32),
            vmem((8, 64, half), BF16),
            vmem((3, 8, 64, half), BF16),
            vmem((8, 4, 64, half), BF16),
            vmem((tokens, 3 * depth), BF16),
            vmem((256, tokens), BF16),
            vmem((2, 3 * depth, half), BF16),
            vmem((2, 3, 2, 2, 128, quarter), BF16),
            vmem((2, 3, 2, 2, 128, quarter), BF16),
            vmem((2, 2, 128, quarter), BF16),
            vmem((2, 2, 128, quarter), BF16),
            vmem((16, 128, width), BF16),
            vmem((128, width), BF16),
            pltpu.SemaphoreType.DMA((120,)),
            pltpu.SemaphoreType.DMA((120,)),
            pltpu.SemaphoreType.DMA((4,)),
            pltpu.SemaphoreType.DMA((4, 2)),
            pltpu.SemaphoreType.DMA((4,)),
            pltpu.SemaphoreType.DMA((4,)),
            pltpu.SemaphoreType.DMA((4, 4)),
            pltpu.SemaphoreType.DMA((4, 4)),
            pltpu.SemaphoreType.DMA((4, 4)),
            pltpu.SemaphoreType.DMA((4, 4)),
            pltpu.SemaphoreType.DMA((4, 2)),
            pltpu.SemaphoreType.DMA((4, 2)),
            pltpu.SemaphoreType.DMA((24,)),
            pltpu.SemaphoreType.DMA((6, 4)),
        ],
        compiler_params=pltpu.CompilerParams(
            collective_id=0, has_side_effects=True, vmem_limit_bytes=66_000_000
        ),
    )(rows, hidden, down_weight, low_feat, mid_feat, join_weight, cotangent)
    return pl.pallas_call(
        deliver,
        out_shape=(
            jax.ShapeDtypeStruct(joined.shape, BF16),
            jax.ShapeDtypeStruct(grad.shape, F32),
        ),
        in_specs=[anywhere] * 2,
        out_specs=(anywhere, anywhere),
        scratch_shapes=[
            vmem(joined.shape, BF16),
            vmem(grad.shape, F32),
            pltpu.SemaphoreType.DMA((2, 7)),
        ],
    )(joined, grad)


def solution(mesh):
    finer = Mesh(mesh.devices.reshape(4, 2, 4, 2, 2), AXES)
    in_specs = (
        P(ROWS, TENSOR),
        P(TENSOR, ROWS),
        P(ROWS, TENSOR),
        P(ROWS, TENSOR),
        P(),
        P(None, TENSOR, ROWS),
        P(TENSOR, ROWS),
    )
    out_specs = (P(TENSOR, ROWS), P(None, TENSOR, ROWS))
    return jax.shard_map(
        on_device, mesh=finer, in_specs=in_specs, out_specs=out_specs, check_vma=False
    )
```

```python
import jax
import jax.numpy as jnp
from jax import lax
from jax.experimental import pallas as pl
from jax.experimental.pallas import tpu as pltpu
from jax.sharding import Mesh
from jax.sharding import PartitionSpec as P

AXES = ("x", "yl", "z", "yh", "c")
ROWS = ("x", "yl")
TENSOR = ("z", "yh", "c")
MESH = pl.DeviceIdType.MESH
F32, BF16 = jnp.float32, jnp.bfloat16
DX = (0, 3, 1, 0, 3, 1, 2, 2)
DY = (0, 0, 0, 1, 1, 1, 0, 1)


def mod4(i):
    return lax.rem(i + 8, 4)


class Copies:
    def __init__(self, send_sems, recv_sems):
        self.send_sems, self.recv_sems, self.made, self.open = send_sems, recv_sems, 0, []

    def send(self, src, dst, to):
        k = self.made
        self.made += 1
        copy = pltpu.make_async_remote_copy(
            src_ref=src,
            dst_ref=dst,
            send_sem=self.send_sems.at[k],
            recv_sem=self.recv_sems.at[k],
            device_id=to,
            device_id_type=MESH,
        )
        copy.start()
        self.open.append(copy)
        return copy

    def drain(self):
        for copy in self.open:
            copy.wait_send()
        self.open = []


class RowGather:
    def __init__(self, copies, buf, src, right, left, across, cut):
        self.send, self.buf, self.src = copies.send, buf, src
        self.right, self.left, self.across = right, left, across
        self.cut, self.mid = cut, 128 + cut // 2

    def own(self):
        b = self.buf
        self.p = self.send(self.src, b.at[3], self.across)
        self.r = self.send(self.src, b.at[1], self.right)
        self.l = self.send(self.src, b.at[2], self.left)

    def partner(self):
        b, cut = self.buf, self.cut
        self.p.wait_recv()
        self.pr = self.send(b.at[3, cut:], b.at[4, cut:], self.right)
        self.pl = self.send(b.at[3, cut:], b.at[5, cut:], self.left)

    def sideways(self):
        b = self.buf
        self.r.wait_recv()
        self.fr = self.send(b.at[1, :128], b.at[6, :128], self.right)
        self.l.wait_recv()
        self.fl = self.send(b.at[2, 128:], b.at[6, 128:], self.left)

    def over(self):
        b, cut = self.buf, self.cut
        self.yl = self.send(b.at[1, :cut], b.at[4, :cut], self.across)
        self.yr = self.send(b.at[2, :cut], b.at[5, :cut], self.across)

    def far(self):
        b, cut, mid = self.buf, self.cut, self.mid
        self.pr.wait_recv()
        self.fpr = self.send(b.at[4, cut:mid], b.at[7, cut:mid], self.right)
        self.pl.wait_recv()
        self.fpl = self.send(b.at[5, mid:], b.at[7, mid:], self.left)

    def sides(self):
        self.yl.wait_recv()
        self.yr.wait_recv()

    def opposite(self):
        b, cut = self.buf, self.cut
        self.fr.wait_recv()
        self.yo = self.send(b.at[6, :cut], b.at[7, :cut], self.across)
        self.fl.wait_recv()

    def last(self):
        self.yo.wait_recv()
        self.fpr.wait_recv()
        self.fpl.wait_recv()


def kernel(
    rows_hbm, hid, w, low, mid, wj, cot,
    joined, grad,
    rows_in, dr, hid_all, w4, lm_all, pq, drecv, drecv2, zr, pr, hp, hx, high, ordered, sel, wjv,
    sb, rb, ys, yr2, cot_all, relay, send_sems, recv_sems, pair_send, pair_recv, over_send,
    over_recv, ring_send, ring_recv, high_send, high_recv, swap_send, swap_recv, local, grad_sems,
):
    x, yl, z, yh, c = (lax.axis_index(a) for a in AXES)
    right, left = (mod4(x + 1), yl, z, yh, c), (mod4(x - 1), yl, z, yh, c)
    across = (x, 1 - yl, z, yh, c)
    up, down = (x, yl, mod4(z + 1), yh, c), (x, yl, mod4(z - 1), yh, c)
    far_y, core = (x, yl, z, 1 - yh, c), (x, yl, z, yh, 1 - c)
    between = (x, 1 - yl, z, 1 - yh, c)
    far_z = (x, yl, mod4(z + 2), yh, c)

    barrier = pltpu.get_barrier_semaphore()
    partners = (right, left, across, between, up, down, far_z, far_y, core)
    for to in partners:
        pl.semaphore_signal(barrier, inc=1, device_id=to, device_id_type=MESH)
    pl.semaphore_wait(barrier, len(partners))
    copies = Copies(send_sems, recv_sems)
    quarter = w4.shape[2]
    half = 2 * quarter
    nlocal = [0]

    def load(src, dst):
        k = nlocal[0]
        nlocal[0] += 1
        copy = pltpu.make_async_copy(src, dst, local.at[k])
        copy.start()
        return copy

    def cb(dz, y, core_at):
        return cot_all.at[mod4(z + dz) * 4 + y * 2 + core_at]

    own_cot = cb(0, yh, c)
    cot_between = copies.send(cot, relay, between)
    hidden = RowGather(copies, hid_all, hid, right, left, across, 96)
    hidden.own()
    loads = [load(hid, hid_all.at[0])]
    for j in range(4):
        at = pl.multiple_of(lax.rem(c + (1 if j < 2 else 0), 2) * half + (j % 2) * quarter, quarter)
        loads.append(load(w.at[:, pl.ds(at, quarter)], w4.at[j]))
    cot_up, cot_down, to_core = copies.send(cot, own_cot, up), copies.send(cot, own_cot, down), []
    to_core.append(copies.send(cot, own_cot, core))
    late = [load(cot, own_cot), load(low, lm_all.at[0, :, 0 : low.shape[1]])]
    late.append(load(mid, lm_all.at[0, :, low.shape[1] :]))
    late.append(load(rows_hbm, rows_in))
    depth = low.shape[1]
    for k in range(3):
        for d in range(2):
            late.append(
                load(wj.at[k, :, d * half : (d + 1) * half], wjv.at[d, k * depth : (k + 1) * depth])
            )
    for copy in loads:
        copy.wait()

    def project(first, stop, which):
        def body(i, _):
            s, j = first + i // 2, i % 2
            pq[which, s, j] = jnp.dot(hid_all[s], w4[which * 2 + j], preferred_element_type=F32)
            return 0

        lax.fori_loop(0, 2 * (stop - first), body, 0)

    to_pair = {}

    def product(first, stop):
        project(first, stop, 0)
        for s in range(first, stop):
            to_pair[s] = copies.send(pq.at[0, s], drecv.at[s], core)
        project(first, stop, 1)

    def pair_sum(first, stop):
        for s in range(first, stop):
            to_pair[s].wait_recv()

        def body(s, _):
            pq[1, s] = pq[1, s] + drecv[s]
            return 0

        lax.fori_loop(first, stop, body, 0)

    def chunk(k):
        return pl.ds(pl.multiple_of(mod4(k) * 64, 64), 64)

    class Sums:
        def __init__(self, group, first, stop):
            self.group, self.first, self.stop = group, first, stop

        def start(self, step):
            f, t = self.first, self.stop
            self.moved = (
                copies.send(pq.at[1, f:t, 0, chunk(z - 1 - step)], zr.at[step, 0, f:t], up),
                copies.send(pq.at[1, f:t, 1, chunk(z + 1 + step)], zr.at[step, 1, f:t], down),
            )

        def add(self, step):
            f, t = self.first, self.stop
            for d, at in ((0, chunk(z - 2 - step)), (1, chunk(z + 2 + step))):
                self.moved[d].wait_recv()
                pq[1, f:t, d, at] = pq[1, f:t, d, at] + zr[step, d, f:t]

        def advance(self, step):
            self.add(step)
            self.start(step + 1)

        def cross(self):
            self.add(2)
            f, t, g = self.first, self.stop, self.group
            self.pair = pltpu.make_async_remote_copy(
                src_ref=pq.at[1, f:t, :, chunk(z)],
                dst_ref=pr.at[yh, f:t],
                send_sem=pair_send.at[g],
                recv_sem=pair_recv.at[g, yh],
                device_id=(x, 1 - yl, z, yl, c),
                device_id_type=MESH,
            )
            self.pair.start()
            self.over = pltpu.make_async_remote_copy(
                src_ref=hp.at[f:t],
                dst_ref=hp.at[f:t],
                send_sem=over_send.at[g],
                recv_sem=over_recv.at[g],
                device_id=across,
                device_id_type=MESH,
            )

        def total(self):
            f, t, g = self.first, self.stop, self.group

            @pl.when(yh != yl)
            def _():
                for n in range(2):
                    pltpu.make_async_remote_copy(
                        src_ref=pr.at[n, f:t],
                        dst_ref=pr.at[n, f:t],
                        send_sem=pair_send.at[g],
                        recv_sem=pair_recv.at[g, n],
                        device_id=across,
                        device_id_type=MESH,
                    ).wait_recv()
                for d in range(2):
                    value = pr[0, f:t, d] + pr[1, f:t, d]
                    hp[f:t, :, d * quarter : (d + 1) * quarter] = value.astype(BF16)
                self.over.start()

        def to_reader(self, n):
            f, t, g = self.first, self.stop, self.group
            src = hp if n == 0 else hx.at[n - 1]
            at = mod4(x + (0, 3, 1, 2)[n])
            copy = pltpu.make_async_remote_copy(
                src_ref=src.at[f:t],
                dst_ref=high.at[f:t, z],
                send_sem=high_send.at[g, n],
                recv_sem=high_recv.at[g, z],
                device_id=(x, yl, at, yh, c),
                device_id_type=MESH,
            )
            return copy, at, src

        def read(self, n):
            f, t = self.first, self.stop
            copy, at, src = self.to_reader(n)
            pl.when(at != z)(copy.start)

            @pl.when(at == z)
            def _():
                high[f:t, z] = src[f:t]

        def ring(self, n, src, dst, to):
            copy = pltpu.make_async_remote_copy(
                src_ref=src,
                dst_ref=dst,
                send_sem=ring_send.at[self.group, n],
                recv_sem=ring_recv.at[self.group, n],
                device_id=to,
                device_id_type=MESH,
            )
            copy.start()
            self.rings.append(copy)

        def publish(self):
            f, t = self.first, self.stop

            @pl.when(yh == yl)
            def _():
                self.over.wait_recv()

            self.rings = []
            self.ring(0, hp.at[f:t], hx.at[0, f:t], right)
            self.ring(1, hp.at[f:t], hx.at[1, f:t], left)
            self.read(0)

        def forward(self):
            f, t = self.first, self.stop
            self.rings[0].wait_recv()
            self.ring(2, hx.at[0, f:t, :32], hx.at[2, f:t, :32], right)
            self.read(1)
            self.rings[1].wait_recv()
            self.ring(3, hx.at[1, f:t, 32:], hx.at[2, f:t, 32:], left)
            self.read(2)

        def finish(self):
            self.rings[2].wait_recv()
            self.rings[3].wait_recv()
            self.read(3)

        def arrive(self):
            f, t, g = self.first, self.stop, self.group
            for i in range(4):
                @pl.when(z != i)
                def _():
                    pltpu.make_async_remote_copy(
                        src_ref=hp.at[f:t],
                        dst_ref=high.at[f:t, i],
                        send_sem=high_send.at[g, 0],
                        recv_sem=high_recv.at[g, i],
                        device_id=core,
                        device_id_type=MESH,
                    ).wait_recv()

        def drain(self):
            self.pair.wait_send()
            pl.when(yh != yl)(self.over.wait_send)
            for copy in self.rings:
                copy.wait_send()
            for n in range(4):
                copy, at, _ = self.to_reader(n)
                pl.when(at != z)(copy.wait_send)

    a, b, e, f = Sums(0, 0, 4), Sums(1, 4, 6), Sums(2, 6, 7), Sums(3, 7, 8)
    groups = (a, b, e, f)

    product(0, 1)
    for copy in late:
        copy.wait()
    cot_half = cot.shape[0] // 2
    ends = []

    def cot_forward(from_down, from_up, y):
        from_down.wait_recv()
        blk = cb(-1, y, c)
        ends.append(copies.send(blk.at[:cot_half], blk.at[:cot_half], up))
        to_core.append(copies.send(blk, blk, core))
        from_up.wait_recv()
        blk = cb(1, y, c)
        ends.append(copies.send(blk.at[cot_half:], blk.at[cot_half:], down))
        to_core.append(copies.send(blk, blk, core))

    for i in range(16):
        lanes = jnp.broadcast_to(rows_in[i : i + 1, :], (128, 128)).astype(F32)
        dr[i * 128 : (i + 1) * 128, :] = lanes.T.astype(jnp.int32)

    def select(row, bx, by):
        rows = dr[pl.ds(row, 256), :]
        lane = lax.broadcasted_iota(jnp.int32, (256, 128), 1)
        for s in range(8):
            base = (mod4(bx + DX[s]) * 2 + lax.rem(by + DY[s], 2)) * 256
            rel = rows - base
            for h in range(2):
                hit = jnp.where(rel == lane + h * 128, 1.0, 0.0).astype(BF16)
                sel[:, s * 256 + h * 128 : s * 256 + (h + 1) * 128] = hit

    wide = lm_all.shape[2]

    def order_lm(first, stop):
        def body(i, _):
            row = pl.multiple_of(i * 256, 256)
            select(row, x, yl)

            def columns(h, _):
                at = pl.ds(pl.multiple_of(h * depth, depth), depth)
                ordered[pl.ds(row, 256), at] = jnp.dot(
                    sel[...], lm_all[:, :, at].reshape(2048, depth), preferred_element_type=F32
                ).astype(BF16)
                return 0

            lax.fori_loop(0, 2, columns, 0)
            return 0

        lax.fori_loop(first, stop, body, 0)

    y_cot = cb(0, 1 - yh, c)
    cot_between.wait_recv()
    cot_forward(cot_up, cot_down, yh)

    hidden.partner()
    hidden.sideways()
    hidden.over()
    cot_over = copies.send(relay, y_cot, across)
    product(1, 4)
    pair_sum(0, 4)
    a.start(0)
    hidden.far()
    a.advance(0)
    hidden.sides()
    product(4, 6)
    hidden.opposite()
    lowmid = RowGather(copies, lm_all, lm_all.at[0], right, left, across, 32)
    lowmid.own()
    pair_sum(4, 6)
    b.start(0)
    a.advance(1)
    product(6, 7)
    b.advance(0)
    pair_sum(6, 7)
    e.start(0)
    hidden.last()
    product(7, 8)
    a.cross()
    pair_sum(7, 8)
    f.start(0)
    b.advance(1)
    e.advance(0)
    f.advance(0)
    lowmid.sideways()
    b.cross()
    e.advance(1)
    lowmid.partner()
    f.advance(1)
    e.cross()
    f.cross()
    lowmid.over()
    lowmid.opposite()
    cot_over.wait_recv()
    ycot_up, ycot_down = copies.send(y_cot, y_cot, up), copies.send(y_cot, y_cot, down)
    to_core.append(copies.send(y_cot, y_cot, core))
    a.total()
    lowmid.far()
    b.total()
    a.publish()
    e.total()
    b.publish()
    f.total()
    e.publish()
    a.forward()
    f.publish()
    lowmid.sides()
    lowmid.last()
    order_lm(0, 2)
    b.forward()
    a.finish()
    cot_forward(ycot_up, ycot_down, 1 - yh)
    order_lm(2, 4)
    e.forward()
    f.forward()
    b.finish()
    order_lm(4, 6)
    e.finish()
    f.finish()
    order_lm(6, 8)
    for copy in ends:
        copy.wait_recv()
    for y in (yh, 1 - yh):
        blk = cb(2, y, c)
        to_core.append(copies.send(blk, blk, core))
    for copy in to_core:
        copy.wait_recv()

    def saving(n, slot, part):
        row = pl.multiple_of(lax.rem(n, depth // 256) * 256, 256)
        return pltpu.make_async_copy(
            drecv.at[slot * 2 + part // 2, part % 2],
            grad.at[n // (depth // 256), pl.ds(row, 256), part * quarter : (part + 1) * quarter],
            grad_sems.at[n, part],
        )

    def gradient(first, stop):
        def body(n, _):
            slot = lax.rem(n, 4)
            features = ordered[:, pl.ds(pl.multiple_of(n * 256, 256), 256)]
            value = lax.dot_general(
                features,
                cot_all[...].reshape(features.shape[0], 2 * half),
                (((0,), (0,)), ((), ())),
                preferred_element_type=F32,
            )
            for part in range(4):
                at = part * quarter
                drecv[slot * 2 + part // 2, part % 2] = value[:, at : at + quarter]
            for part in range(4):
                saving(n, slot, part).start()
            return 0

        lax.fori_loop(first, stop, body, 0)

    def saved(first, stop):
        for n in range(first, stop):
            for part in range(4):
                saving(n, n % 4, part).wait()

    gradient(0, 2)
    for g in groups:
        g.arrive()
    for g in groups:
        g.drain()
    copies.drain()

    ring_at = (mod4(z - 1), mod4(z + 1), mod4(z + 2), z)

    def order_high(i):
        def body(n, _):
            row = pl.multiple_of(ring_at[i] * 512 + n * 256, 256)
            select(row, z, yh)
            ordered[pl.ds(row, 256), wide:] = jnp.dot(
                sel[...], high[...].reshape(2048, half), preferred_element_type=F32
            ).astype(BF16)
            return 0

        lax.fori_loop(0, 2, body, 0)

    paired = {}

    def join(i, d):
        def part(which, _):
            side = lax.rem(c + 1 - which, 2)
            at = pl.multiple_of(ring_at[i] * 512 + side * 128, 128)
            rows = jnp.concatenate(
                [ordered[pl.ds(at, 128), :], ordered[pl.ds(at + 256, 128), :]], axis=0
            )
            value = jnp.dot(rows, wjv[d], preferred_element_type=F32)
            pq[which, 2 * i + d, 0] = value[:, :quarter]
            pq[which, 2 * i + d, 1] = value[:, quarter:]

            @pl.when(which == 0)
            def _():
                swap(i, d).start()

            return 0

        lax.fori_loop(0, 2, part, 0)
        paired[i, d] = swap(i, d)

    def swap(i, d):
        return pltpu.make_async_remote_copy(
            src_ref=pq.at[0, 2 * i + d],
            dst_ref=drecv2.at[2 * i + d],
            send_sem=swap_send.at[i, d],
            recv_sem=swap_recv.at[i, d],
            device_id=core,
            device_id_type=MESH,
        )

    streams = (1 - yh, yh)
    turns = ((0, 2, 1, 3), (1, 2, 0, 3))

    def both(i, d, st):
        at = pl.ds(pl.multiple_of(streams[st] * 128, 128), 128)
        return pq[1, 2 * i + d, :, at] + drecv2[2 * i + d, :, at]

    moving = {}

    def turn(step, d, st):
        value = both(turns[d][step], d, st)
        if step:
            moving[step - 1, d, st].wait_recv()
            value = value + rb[d, step - 1, st].astype(F32)
        if step < 3:
            sb[d, step, st] = value.astype(BF16)
            to = up if d == 0 else down
            moving[step, d, st] = copies.send(sb.at[d, step, st], rb.at[d, step, st], to)
        return value

    order_high(0)
    join(0, 0)
    order_high(1)
    join(1, 1)
    paired[0, 0].wait_recv()
    turn(0, 0, 0)
    turn(0, 0, 1)
    paired[1, 1].wait_recv()
    turn(0, 1, 0)
    turn(0, 1, 1)
    order_high(2)
    join(2, 0)
    join(2, 1)
    join(1, 0)
    paired[2, 0].wait_recv()
    paired[2, 1].wait_recv()
    for st in range(2):
        for d in range(2):
            turn(1, d, st)
    join(0, 1)
    order_high(3)
    join(3, 0)
    join(3, 1)
    paired[1, 0].wait_recv()
    paired[0, 1].wait_recv()
    for st in range(2):
        for d in range(2):
            turn(2, d, st)
    gradient(2, 4)
    paired[3, 0].wait_recv()
    paired[3, 1].wait_recv()
    ys[1] = turn(3, 1, 0).astype(ys.dtype)
    relayed = copies.send(ys.at[1], yr2.at[2], between)
    ys[0] = turn(3, 0, 0).astype(ys.dtype)
    direct = copies.send(ys.at[0], yr2.at[0], far_y)
    final = [turn(3, d, 1) for d in range(2)]
    relayed.wait_recv()
    last = copies.send(yr2.at[2], yr2.at[1], across)
    saved(0, 2)
    gradient(4, 6)
    direct.wait_recv()
    last.wait_recv()
    for d in range(2):
        value = (final[d] + yr2[d].astype(F32)).astype(BF16)
        for h in range(2):
            at = d * half + h * quarter
            joined[:, at : at + quarter] = value[h]
    copies.drain()
    for copy in paired.values():
        copy.wait_send()
    saved(2, 6)


def deliver(joined, grad, joined_out, grad_out, joined_buf, grad_buf, sems):
    blocks = [(joined, joined_buf, joined_out)]
    rows = grad.shape[1] // 2
    for k in range(3):
        for h in range(2):
            at = (k, pl.ds(h * rows, rows))
            blocks.append((grad.at[at], grad_buf.at[at], grad_out.at[at]))
    loads = [pltpu.make_async_copy(s, b, sems.at[0, n]) for n, (s, b, _) in enumerate(blocks)]
    stores = [pltpu.make_async_copy(b, o, sems.at[1, n]) for n, (_, b, o) in enumerate(blocks)]
    for copy in loads:
        copy.start()
    for copy, store in zip(loads, stores):
        copy.wait()
        store.start()
    for store in stores:
        store.wait()


def on_device(hidden, down_weight, low_feat, mid_feat, draft_rows, join_weight, cotangent):
    tokens = draft_rows.shape[0]
    units, width = down_weight.shape
    depth = low_feat.shape[1]
    half, quarter = width // 2, width // 4
    rows = draft_rows.reshape(tokens // 128, 128)
    anywhere = pl.BlockSpec(memory_space=pl.ANY)
    vmem = pltpu.VMEM
    joined, grad = pl.pallas_call(
        kernel,
        out_shape=(
            jax.ShapeDtypeStruct((128, width), BF16),
            jax.ShapeDtypeStruct((3, depth, width), F32),
        ),
        in_specs=[anywhere] * 7,
        out_specs=(pl.BlockSpec(memory_space=vmem), anywhere),
        scratch_shapes=[
            vmem((tokens // 128, 128), jnp.int32),
            vmem((tokens, 128), jnp.int32),
            vmem((8, 256, units), BF16),
            vmem((4, units, quarter), BF16),
            vmem((8, 256, 2 * depth), BF16),
            vmem((2, 8, 2, 256, quarter), F32),
            vmem((8, 2, 256, quarter), F32),
            vmem((8, 2, 256, quarter), F32),
            vmem((3, 2, 8, 64, quarter), F32),
            vmem((2, 8, 2, 64, quarter), F32),
            vmem((8, 64, half), BF16),
            vmem((3, 8, 64, half), BF16),
            vmem((8, 4, 64, half), BF16),
            vmem((tokens, 3 * depth), BF16),
            vmem((256, tokens), BF16),
            vmem((2, 3 * depth, half), BF16),
            vmem((2, 3, 2, 2, 128, quarter), BF16),
            vmem((2, 3, 2, 2, 128, quarter), BF16),
            vmem((2, 2, 128, quarter), BF16),
            vmem((3, 2, 128, quarter), BF16),
            vmem((16, 128, width), BF16),
            vmem((128, width), BF16),
            pltpu.SemaphoreType.DMA((120,)),
            pltpu.SemaphoreType.DMA((120,)),
            pltpu.SemaphoreType.DMA((4,)),
            pltpu.SemaphoreType.DMA((4, 2)),
            pltpu.SemaphoreType.DMA((4,)),
            pltpu.SemaphoreType.DMA((4,)),
            pltpu.SemaphoreType.DMA((4, 4)),
            pltpu.SemaphoreType.DMA((4, 4)),
            pltpu.SemaphoreType.DMA((4, 4)),
            pltpu.SemaphoreType.DMA((4, 4)),
            pltpu.SemaphoreType.DMA((4, 2)),
            pltpu.SemaphoreType.DMA((4, 2)),
            pltpu.SemaphoreType.DMA((24,)),
            pltpu.SemaphoreType.DMA((6, 4)),
        ],
        compiler_params=pltpu.CompilerParams(
            collective_id=0, has_side_effects=True, vmem_limit_bytes=66_000_000
        ),
    )(rows, hidden, down_weight, low_feat, mid_feat, join_weight, cotangent)
    return pl.pallas_call(
        deliver,
        out_shape=(
            jax.ShapeDtypeStruct(joined.shape, BF16),
            jax.ShapeDtypeStruct(grad.shape, F32),
        ),
        in_specs=[anywhere] * 2,
        out_specs=(anywhere, anywhere),
        scratch_shapes=[
            vmem(joined.shape, BF16),
            vmem(grad.shape, F32),
            pltpu.SemaphoreType.DMA((2, 7)),
        ],
    )(joined, grad)


def solution(mesh):
    finer = Mesh(mesh.devices.reshape(4, 2, 4, 2, 2), AXES)
    in_specs = (
        P(ROWS, TENSOR),
        P(TENSOR, ROWS),
        P(ROWS, TENSOR),
        P(ROWS, TENSOR),
        P(),
        P(None, TENSOR, ROWS),
        P(TENSOR, ROWS),
    )
    out_specs = (P(TENSOR, ROWS), P(None, TENSOR, ROWS))
    return jax.shard_map(
        on_device, mesh=finer, in_specs=in_specs, out_specs=out_specs, check_vma=False
    )
```

```python
import jax
import jax.numpy as jnp
from jax import lax
from jax.experimental import pallas as pl
from jax.experimental.pallas import tpu as pltpu
from jax.sharding import Mesh
from jax.sharding import PartitionSpec as P

AXES = ("x", "yl", "z", "yh", "c")
ROWS = ("x", "yl")
TENSOR = ("z", "yh", "c")
MESH = pl.DeviceIdType.MESH
F32, BF16 = jnp.float32, jnp.bfloat16
DX = (0, 3, 1, 0, 3, 1, 2, 2)
DY = (0, 0, 0, 1, 1, 1, 0, 1)


def mod4(i):
    return lax.rem(i + 8, 4)


class Copies:
    def __init__(self, send_sems, recv_sems):
        self.send_sems, self.recv_sems, self.made, self.open = send_sems, recv_sems, 0, []

    def send(self, src, dst, to):
        k = self.made
        self.made += 1
        copy = pltpu.make_async_remote_copy(
            src_ref=src,
            dst_ref=dst,
            send_sem=self.send_sems.at[k],
            recv_sem=self.recv_sems.at[k],
            device_id=to,
            device_id_type=MESH,
        )
        copy.start()
        self.open.append(copy)
        return copy

    def drain(self):
        for copy in self.open:
            copy.wait_send()
        self.open = []


class RowGather:
    def __init__(self, copies, buf, src, right, left, across, cut):
        self.send, self.buf, self.src = copies.send, buf, src
        self.right, self.left, self.across = right, left, across
        self.cut, self.mid = cut, 128 + cut // 2

    def own(self):
        b = self.buf
        self.r = self.send(self.src, b.at[1], self.right)
        self.l = self.send(self.src, b.at[2], self.left)

    def own_over(self):
        self.p = self.send(self.src, self.buf.at[3], self.across)

    def partner(self):
        b, cut = self.buf, self.cut
        self.p.wait_recv()
        self.pr = self.send(b.at[3, cut:], b.at[4, cut:], self.right)
        self.pl = self.send(b.at[3, cut:], b.at[5, cut:], self.left)

    def sideways(self):
        b = self.buf
        self.r.wait_recv()
        self.fr = self.send(b.at[1, :128], b.at[6, :128], self.right)
        self.l.wait_recv()
        self.fl = self.send(b.at[2, 128:], b.at[6, 128:], self.left)

    def over(self):
        b, cut = self.buf, self.cut
        self.yl = self.send(b.at[1, :cut], b.at[4, :cut], self.across)
        self.yr = self.send(b.at[2, :cut], b.at[5, :cut], self.across)

    def far(self):
        b, cut, mid = self.buf, self.cut, self.mid
        self.pr.wait_recv()
        self.fpr = self.send(b.at[4, cut:mid], b.at[7, cut:mid], self.right)
        self.pl.wait_recv()
        self.fpl = self.send(b.at[5, mid:], b.at[7, mid:], self.left)

    def sides(self):
        self.yl.wait_recv()
        self.yr.wait_recv()

    def opposite(self):
        b, cut = self.buf, self.cut
        self.fr.wait_recv()
        self.yo = self.send(b.at[6, :cut], b.at[7, :cut], self.across)
        self.fl.wait_recv()

    def last(self):
        self.yo.wait_recv()
        self.fpr.wait_recv()
        self.fpl.wait_recv()


def kernel(
    rows_hbm, hid, w, low, mid, wj, cot,
    joined, grad,
    rows_in, dr, hid_all, w4, low_all, mid_all, pq, drecv, drecv2, zr, pr, hp, hx, high, ordered, sel, wjv,
    sb, rb, ys, yr2, cot_all, relay, send_sems, recv_sems, pair_send, pair_recv, over_send,
    over_recv, ring_send, ring_recv, high_send, high_recv, swap_send, swap_recv, local, grad_sems,
):
    x, yl, z, yh, c = (lax.axis_index(a) for a in AXES)
    right, left = (mod4(x + 1), yl, z, yh, c), (mod4(x - 1), yl, z, yh, c)
    across = (x, 1 - yl, z, yh, c)
    up, down = (x, yl, mod4(z + 1), yh, c), (x, yl, mod4(z - 1), yh, c)
    far_y, core = (x, yl, z, 1 - yh, c), (x, yl, z, yh, 1 - c)
    between = (x, 1 - yl, z, 1 - yh, c)
    far_z = (x, yl, mod4(z + 2), yh, c)

    barrier = pltpu.get_barrier_semaphore()
    partners = (right, left, across, between, up, down, far_z, far_y, core)
    for to in partners:
        pl.semaphore_signal(barrier, inc=1, device_id=to, device_id_type=MESH)
    pl.semaphore_wait(barrier, len(partners))
    copies = Copies(send_sems, recv_sems)
    quarter = w4.shape[2]
    half = 2 * quarter
    nlocal = [0]

    def load(src, dst):
        k = nlocal[0]
        nlocal[0] += 1
        copy = pltpu.make_async_copy(src, dst, local.at[k])
        copy.start()
        return copy

    def cb(dz, y, core_at):
        return cot_all.at[mod4(z + dz) * 4 + y * 2 + core_at]

    own_cot = cb(0, yh, c)
    cot_between = copies.send(cot, relay, between)
    hidden = RowGather(copies, hid_all, hid, right, left, across, 96)
    hidden.own_over()
    hidden.own()
    loads = [load(hid, hid_all.at[0])]
    for j in range(4):
        at = pl.multiple_of(lax.rem(c + (1 if j < 2 else 0), 2) * half + (j % 2) * quarter, quarter)
        loads.append(load(w.at[:, pl.ds(at, quarter)], w4.at[j]))
    cot_up, cot_down, to_core = copies.send(cot, own_cot, up), copies.send(cot, own_cot, down), []
    to_core.append(copies.send(cot, own_cot, core))
    late = [load(cot, own_cot), load(low, low_all.at[0]), load(mid, mid_all.at[0])]
    late.append(load(rows_hbm, rows_in))
    depth = low.shape[1]
    for k in range(3):
        for d in range(2):
            late.append(
                load(wj.at[k, :, d * half : (d + 1) * half], wjv.at[d, k * depth : (k + 1) * depth])
            )
    for copy in loads:
        copy.wait()

    def project(first, stop, which):
        def body(i, _):
            s, j = first + i // 2, i % 2
            pq[which, s, j] = jnp.dot(hid_all[s], w4[which * 2 + j], preferred_element_type=F32)
            return 0

        lax.fori_loop(0, 2 * (stop - first), body, 0)

    to_pair = {}

    def product(first, stop):
        project(first, stop, 0)
        for s in range(first, stop):
            to_pair[s] = copies.send(pq.at[0, s], drecv.at[s], core)
        project(first, stop, 1)

    def pair_sum(first, stop):
        for s in range(first, stop):
            to_pair[s].wait_recv()

        def body(s, _):
            pq[1, s] = pq[1, s] + drecv[s]
            return 0

        lax.fori_loop(first, stop, body, 0)

    def chunk(k):
        return pl.ds(pl.multiple_of(mod4(k) * 64, 64), 64)

    class Sums:
        def __init__(self, group, first, stop):
            self.group, self.first, self.stop = group, first, stop

        def start(self, step):
            f, t = self.first, self.stop
            self.moved = (
                copies.send(pq.at[1, f:t, 0, chunk(z - 1 - step)], zr.at[step, 0, f:t], up),
                copies.send(pq.at[1, f:t, 1, chunk(z + 1 + step)], zr.at[step, 1, f:t], down),
            )

        def add(self, step):
            f, t = self.first, self.stop
            for d, at in ((0, chunk(z - 2 - step)), (1, chunk(z + 2 + step))):
                self.moved[d].wait_recv()
                pq[1, f:t, d, at] = pq[1, f:t, d, at] + zr[step, d, f:t]

        def advance(self, step):
            self.add(step)
            self.start(step + 1)

        def cross(self):
            self.add(2)
            f, t, g = self.first, self.stop, self.group
            self.pair = pltpu.make_async_remote_copy(
                src_ref=pq.at[1, f:t, :, chunk(z)],
                dst_ref=pr.at[yh, f:t],
                send_sem=pair_send.at[g],
                recv_sem=pair_recv.at[g, yh],
                device_id=(x, 1 - yl, z, yl, c),
                device_id_type=MESH,
            )
            self.pair.start()
            self.over = pltpu.make_async_remote_copy(
                src_ref=hp.at[f:t],
                dst_ref=hp.at[f:t],
                send_sem=over_send.at[g],
                recv_sem=over_recv.at[g],
                device_id=across,
                device_id_type=MESH,
            )

        def total(self):
            f, t, g = self.first, self.stop, self.group

            @pl.when(yh != yl)
            def _():
                for n in range(2):
                    pltpu.make_async_remote_copy(
                        src_ref=pr.at[n, f:t],
                        dst_ref=pr.at[n, f:t],
                        send_sem=pair_send.at[g],
                        recv_sem=pair_recv.at[g, n],
                        device_id=across,
                        device_id_type=MESH,
                    ).wait_recv()
                for d in range(2):
                    value = pr[0, f:t, d] + pr[1, f:t, d]
                    hp[f:t, :, d * quarter : (d + 1) * quarter] = value.astype(BF16)
                self.over.start()

        def to_reader(self, n):
            f, t, g = self.first, self.stop, self.group
            src = hp if n == 0 else hx.at[n - 1]
            at = mod4(x + (0, 3, 1, 2)[n])
            copy = pltpu.make_async_remote_copy(
                src_ref=src.at[f:t],
                dst_ref=high.at[f:t, z],
                send_sem=high_send.at[g, n],
                recv_sem=high_recv.at[g, z],
                device_id=(x, yl, at, yh, c),
                device_id_type=MESH,
            )
            return copy, at, src

        def read(self, n):
            f, t = self.first, self.stop
            copy, at, src = self.to_reader(n)
            pl.when(at != z)(copy.start)

            @pl.when(at == z)
            def _():
                high[f:t, z] = src[f:t]

        def ring(self, n, src, dst, to):
            copy = pltpu.make_async_remote_copy(
                src_ref=src,
                dst_ref=dst,
                send_sem=ring_send.at[self.group, n],
                recv_sem=ring_recv.at[self.group, n],
                device_id=to,
                device_id_type=MESH,
            )
            copy.start()
            self.rings.append(copy)

        def publish(self):
            f, t = self.first, self.stop

            @pl.when(yh == yl)
            def _():
                self.over.wait_recv()

            self.rings = []
            self.ring(0, hp.at[f:t], hx.at[0, f:t], right)
            self.ring(1, hp.at[f:t], hx.at[1, f:t], left)
            self.read(0)

        def forward(self):
            f, t = self.first, self.stop
            self.rings[0].wait_recv()
            self.ring(2, hx.at[0, f:t, :32], hx.at[2, f:t, :32], right)
            self.read(1)
            self.rings[1].wait_recv()
            self.ring(3, hx.at[1, f:t, 32:], hx.at[2, f:t, 32:], left)
            self.read(2)

        def finish(self):
            self.rings[2].wait_recv()
            self.rings[3].wait_recv()
            self.read(3)

        def arrive(self):
            f, t, g = self.first, self.stop, self.group
            for i in range(4):
                @pl.when(z != i)
                def _():
                    pltpu.make_async_remote_copy(
                        src_ref=hp.at[f:t],
                        dst_ref=high.at[f:t, i],
                        send_sem=high_send.at[g, 0],
                        recv_sem=high_recv.at[g, i],
                        device_id=core,
                        device_id_type=MESH,
                    ).wait_recv()

        def drain(self):
            self.pair.wait_send()
            pl.when(yh != yl)(self.over.wait_send)
            for copy in self.rings:
                copy.wait_send()
            for n in range(4):
                copy, at, _ = self.to_reader(n)
                pl.when(at != z)(copy.wait_send)

    a, b, e, f = Sums(0, 0, 4), Sums(1, 4, 6), Sums(2, 6, 7), Sums(3, 7, 8)
    groups = (a, b, e, f)

    product(0, 1)
    for copy in late:
        copy.wait()
    cot_half = cot.shape[0] // 2
    ends = []

    def cot_forward(from_down, from_up, y):
        from_down.wait_recv()
        blk = cb(-1, y, c)
        ends.append(copies.send(blk.at[:cot_half], blk.at[:cot_half], up))
        to_core.append(copies.send(blk, blk, core))
        from_up.wait_recv()
        blk = cb(1, y, c)
        ends.append(copies.send(blk.at[cot_half:], blk.at[cot_half:], down))
        to_core.append(copies.send(blk, blk, core))

    for i in range(16):
        lanes = jnp.broadcast_to(rows_in[i : i + 1, :], (128, 128)).astype(F32)
        dr[i * 128 : (i + 1) * 128, :] = lanes.T.astype(jnp.int32)

    def select(row, bx, by):
        rows = dr[pl.ds(row, 256), :]
        lane = lax.broadcasted_iota(jnp.int32, (256, 128), 1)
        for s in range(8):
            base = (mod4(bx + DX[s]) * 2 + lax.rem(by + DY[s], 2)) * 256
            rel = rows - base
            for h in range(2):
                hit = jnp.where(rel == lane + h * 128, 1.0, 0.0).astype(BF16)
                sel[:, s * 256 + h * 128 : s * 256 + (h + 1) * 128] = hit

    wide = 2 * depth

    def order(features, at, first, stop):
        def body(i, _):
            row = pl.multiple_of(i * 256, 256)
            select(row, x, yl)
            ordered[pl.ds(row, 256), at : at + depth] = jnp.dot(
                sel[...], features[...].reshape(2048, depth), preferred_element_type=F32
            ).astype(BF16)
            return 0

        lax.fori_loop(first, stop, body, 0)

    y_cot = cb(0, 1 - yh, c)
    cot_between.wait_recv()
    cot_forward(cot_up, cot_down, yh)

    hidden.partner()
    hidden.sideways()
    hidden.over()
    cot_over = copies.send(relay, y_cot, across)
    lows = RowGather(copies, low_all, low_all.at[0], right, left, across, 32)
    mids = RowGather(copies, mid_all, mid_all.at[0], right, left, across, 32)
    product(1, 4)
    pair_sum(0, 4)
    a.start(0)
    hidden.far()
    lows.own()
    mids.own()
    a.advance(0)
    hidden.sides()
    product(4, 6)
    hidden.opposite()
    lows.own_over()
    mids.own_over()
    pair_sum(4, 6)
    b.start(0)
    a.advance(1)
    product(6, 7)
    b.advance(0)
    pair_sum(6, 7)
    e.start(0)
    a.cross()
    b.advance(1)
    e.advance(0)
    hidden.last()
    product(7, 8)
    b.cross()
    pair_sum(7, 8)
    f.start(0)
    lows.sideways()
    lows.partner()
    e.advance(1)
    f.advance(0)
    mids.sideways()
    mids.partner()
    e.cross()
    f.advance(1)
    f.cross()
    cot_over.wait_recv()
    ycot_up, ycot_down = copies.send(y_cot, y_cot, up), copies.send(y_cot, y_cot, down)
    to_core.append(copies.send(y_cot, y_cot, core))
    a.total()
    a.publish()
    lows.over()
    lows.opposite()
    lows.far()
    b.total()
    b.publish()
    mids.over()
    mids.opposite()
    mids.far()
    a.forward()
    e.total()
    e.publish()
    b.forward()
    f.total()
    f.publish()
    a.finish()
    lows.sides()
    lows.last()
    cot_forward(ycot_up, ycot_down, 1 - yh)
    e.forward()
    b.finish()
    order(low_all, 0, 0, 4)
    f.forward()
    e.finish()
    order(low_all, 0, 4, 8)
    f.finish()
    mids.sides()
    mids.last()
    order(mid_all, depth, 0, 8)
    for copy in ends:
        copy.wait_recv()
    for y in (yh, 1 - yh):
        blk = cb(2, y, c)
        to_core.append(copies.send(blk, blk, core))
    for copy in to_core:
        copy.wait_recv()

    def saving(n, slot, part):
        row = pl.multiple_of(lax.rem(n, depth // 256) * 256, 256)
        return pltpu.make_async_copy(
            drecv.at[slot * 2 + part // 2, part % 2],
            grad.at[n // (depth // 256), pl.ds(row, 256), part * quarter : (part + 1) * quarter],
            grad_sems.at[n, part],
        )

    def gradient(first, stop):
        def body(n, _):
            slot = lax.rem(n, 4)
            features = ordered[:, pl.ds(pl.multiple_of(n * 256, 256), 256)]
            value = lax.dot_general(
                features,
                cot_all[...].reshape(features.shape[0], 2 * half),
                (((0,), (0,)), ((), ())),
                preferred_element_type=F32,
            )
            for part in range(4):
                at = part * quarter
                drecv[slot * 2 + part // 2, part % 2] = value[:, at : at + quarter]
            for part in range(4):
                saving(n, slot, part).start()
            return 0

        lax.fori_loop(first, stop, body, 0)

    def saved(first, stop):
        for n in range(first, stop):
            for part in range(4):
                saving(n, n % 4, part).wait()

    for g in groups:
        g.arrive()
    for g in groups:
        g.drain()
    copies.drain()

    ring_at = (mod4(z - 1), mod4(z + 1), mod4(z + 2), z)

    def order_high(i):
        def body(n, _):
            row = pl.multiple_of(ring_at[i] * 512 + n * 256, 256)
            select(row, z, yh)
            ordered[pl.ds(row, 256), wide:] = jnp.dot(
                sel[...], high[...].reshape(2048, half), preferred_element_type=F32
            ).astype(BF16)
            return 0

        lax.fori_loop(0, 2, body, 0)

    paired = {}

    def join(i, d):
        def part(which, _):
            side = lax.rem(c + 1 - which, 2)
            at = pl.multiple_of(ring_at[i] * 512 + side * 128, 128)
            rows = jnp.concatenate(
                [ordered[pl.ds(at, 128), :], ordered[pl.ds(at + 256, 128), :]], axis=0
            )
            value = jnp.dot(rows, wjv[d], preferred_element_type=F32)
            pq[which, 2 * i + d, 0] = value[:, :quarter]
            pq[which, 2 * i + d, 1] = value[:, quarter:]

            @pl.when(which == 0)
            def _():
                swap(i, d).start()

            return 0

        lax.fori_loop(0, 2, part, 0)
        paired[i, d] = swap(i, d)

    def swap(i, d):
        return pltpu.make_async_remote_copy(
            src_ref=pq.at[0, 2 * i + d],
            dst_ref=drecv2.at[2 * i + d],
            send_sem=swap_send.at[i, d],
            recv_sem=swap_recv.at[i, d],
            device_id=core,
            device_id_type=MESH,
        )

    streams = (1 - yh, yh)
    turns = ((0, 2, 1, 3), (1, 2, 0, 3))

    def both(i, d, st):
        at = pl.ds(pl.multiple_of(streams[st] * 128, 128), 128)
        return pq[1, 2 * i + d, :, at] + drecv2[2 * i + d, :, at]

    moving = {}

    def turn(step, d, st):
        value = both(turns[d][step], d, st)
        if step:
            moving[step - 1, d, st].wait_recv()
            value = value + rb[d, step - 1, st].astype(F32)
        if step < 3:
            sb[d, step, st] = value.astype(BF16)
            to = up if d == 0 else down
            moving[step, d, st] = copies.send(sb.at[d, step, st], rb.at[d, step, st], to)
        return value

    order_high(0)
    join(0, 0)
    order_high(1)
    join(1, 1)
    paired[0, 0].wait_recv()
    turn(0, 0, 0)
    turn(0, 0, 1)
    paired[1, 1].wait_recv()
    turn(0, 1, 0)
    turn(0, 1, 1)
    order_high(2)
    join(2, 0)
    join(2, 1)
    join(1, 0)
    paired[2, 0].wait_recv()
    paired[2, 1].wait_recv()
    for st in range(2):
        for d in range(2):
            turn(1, d, st)
    join(0, 1)
    order_high(3)
    join(3, 0)
    join(3, 1)
    paired[1, 0].wait_recv()
    paired[0, 1].wait_recv()
    for st in range(2):
        for d in range(2):
            turn(2, d, st)
    gradient(2, 4)
    paired[3, 0].wait_recv()
    paired[3, 1].wait_recv()
    for d in range(2):
        ys[d] = turn(3, d, 0).astype(ys.dtype)
    last = copies.send(ys, yr2, far_y)
    final = [turn(3, d, 1) for d in range(2)]
    gradient(0, 2)
    saved(0, 2)
    gradient(4, 6)
    last.wait_recv()
    for d in range(2):
        value = (final[d] + yr2[d].astype(F32)).astype(BF16)
        for h in range(2):
            at = d * half + h * quarter
            joined[:, at : at + quarter] = value[h]
    copies.drain()
    for copy in paired.values():
        copy.wait_send()
    saved(2, 6)


def deliver(joined, grad, joined_out, grad_out, joined_buf, grad_buf, sems):
    blocks = [(joined, joined_buf, joined_out)]
    rows = grad.shape[1] // 2
    for k in range(3):
        for h in range(2):
            at = (k, pl.ds(h * rows, rows))
            blocks.append((grad.at[at], grad_buf.at[at], grad_out.at[at]))
    loads = [pltpu.make_async_copy(s, b, sems.at[0, n]) for n, (s, b, _) in enumerate(blocks)]
    stores = [pltpu.make_async_copy(b, o, sems.at[1, n]) for n, (_, b, o) in enumerate(blocks)]
    for copy in loads:
        copy.start()
    for copy, store in zip(loads, stores):
        copy.wait()
        store.start()
    for store in stores:
        store.wait()


def on_device(hidden, down_weight, low_feat, mid_feat, draft_rows, join_weight, cotangent):
    tokens = draft_rows.shape[0]
    units, width = down_weight.shape
    depth = low_feat.shape[1]
    half, quarter = width // 2, width // 4
    rows = draft_rows.reshape(tokens // 128, 128)
    anywhere = pl.BlockSpec(memory_space=pl.ANY)
    vmem = pltpu.VMEM
    joined, grad = pl.pallas_call(
        kernel,
        out_shape=(
            jax.ShapeDtypeStruct((128, width), BF16),
            jax.ShapeDtypeStruct((3, depth, width), F32),
        ),
        in_specs=[anywhere] * 7,
        out_specs=(pl.BlockSpec(memory_space=vmem), anywhere),
        scratch_shapes=[
            vmem((tokens // 128, 128), jnp.int32),
            vmem((tokens, 128), jnp.int32),
            vmem((8, 256, units), BF16),
            vmem((4, units, quarter), BF16),
            vmem((8, 256, depth), BF16),
            vmem((8, 256, depth), BF16),
            vmem((2, 8, 2, 256, quarter), F32),
            vmem((8, 2, 256, quarter), F32),
            vmem((8, 2, 256, quarter), F32),
            vmem((3, 2, 8, 64, quarter), F32),
            vmem((2, 8, 2, 64, quarter), F32),
            vmem((8, 64, half), BF16),
            vmem((3, 8, 64, half), BF16),
            vmem((8, 4, 64, half), BF16),
            vmem((tokens, 3 * depth), BF16),
            vmem((256, tokens), BF16),
            vmem((2, 3 * depth, half), BF16),
            vmem((2, 3, 2, 2, 128, quarter), BF16),
            vmem((2, 3, 2, 2, 128, quarter), BF16),
            vmem((2, 2, 128, quarter), BF16),
            vmem((2, 2, 128, quarter), BF16),
            vmem((16, 128, width), BF16),
            vmem((128, width), BF16),
            pltpu.SemaphoreType.DMA((120,)),
            pltpu.SemaphoreType.DMA((120,)),
            pltpu.SemaphoreType.DMA((4,)),
            pltpu.SemaphoreType.DMA((4, 2)),
            pltpu.SemaphoreType.DMA((4,)),
            pltpu.SemaphoreType.DMA((4,)),
            pltpu.SemaphoreType.DMA((4, 4)),
            pltpu.SemaphoreType.DMA((4, 4)),
            pltpu.SemaphoreType.DMA((4, 4)),
            pltpu.SemaphoreType.DMA((4, 4)),
            pltpu.SemaphoreType.DMA((4, 2)),
            pltpu.SemaphoreType.DMA((4, 2)),
            pltpu.SemaphoreType.DMA((24,)),
            pltpu.SemaphoreType.DMA((6, 4)),
        ],
        compiler_params=pltpu.CompilerParams(
            collective_id=0, has_side_effects=True, vmem_limit_bytes=66_000_000
        ),
    )(rows, hidden, down_weight, low_feat, mid_feat, join_weight, cotangent)
    return pl.pallas_call(
        deliver,
        out_shape=(
            jax.ShapeDtypeStruct(joined.shape, BF16),
            jax.ShapeDtypeStruct(grad.shape, F32),
        ),
        in_specs=[anywhere] * 2,
        out_specs=(anywhere, anywhere),
        scratch_shapes=[
            vmem(joined.shape, BF16),
            vmem(grad.shape, F32),
            pltpu.SemaphoreType.DMA((2, 7)),
        ],
    )(joined, grad)


def solution(mesh):
    finer = Mesh(mesh.devices.reshape(4, 2, 4, 2, 2), AXES)
    in_specs = (
        P(ROWS, TENSOR),
        P(TENSOR, ROWS),
        P(ROWS, TENSOR),
        P(ROWS, TENSOR),
        P(),
        P(None, TENSOR, ROWS),
        P(TENSOR, ROWS),
    )
    out_specs = (P(TENSOR, ROWS), P(None, TENSOR, ROWS))
    return jax.shard_map(
        on_device, mesh=finer, in_specs=in_specs, out_specs=out_specs, check_vma=False
    )
```

```python
import jax
import jax.numpy as jnp
from jax import lax
from jax.experimental import pallas as pl
from jax.experimental.pallas import tpu as pltpu
from jax.sharding import Mesh
from jax.sharding import PartitionSpec as P

AXES = ("x", "yl", "z", "yh", "c")
ROWS = ("x", "yl")
TENSOR = ("z", "yh", "c")
MESH = pl.DeviceIdType.MESH
F32, BF16 = jnp.float32, jnp.bfloat16
DX = (0, 3, 1, 0, 3, 1, 2, 2)
DY = (0, 0, 0, 1, 1, 1, 0, 1)


def mod4(i):
    return lax.rem(i + 8, 4)


class Copies:
    def __init__(self, send_sems, recv_sems):
        self.send_sems, self.recv_sems, self.made, self.open = send_sems, recv_sems, 0, []

    def send(self, src, dst, to):
        k = self.made
        self.made += 1
        copy = pltpu.make_async_remote_copy(
            src_ref=src,
            dst_ref=dst,
            send_sem=self.send_sems.at[k],
            recv_sem=self.recv_sems.at[k],
            device_id=to,
            device_id_type=MESH,
        )
        copy.start()
        self.open.append(copy)
        return copy

    def drain(self):
        for copy in self.open:
            copy.wait_send()
        self.open = []


class RowGather:
    def __init__(self, copies, buf, src, right, left, across, cut):
        self.send, self.buf, self.src = copies.send, buf, src
        self.right, self.left, self.across = right, left, across
        self.cut, self.mid = cut, 128 + cut // 2

    def own(self):
        b = self.buf
        self.r = self.send(self.src, b.at[1], self.right)
        self.l = self.send(self.src, b.at[2], self.left)

    def own_over(self):
        self.p = self.send(self.src, self.buf.at[3], self.across)

    def partner(self):
        b, cut = self.buf, self.cut
        self.p.wait_recv()
        self.pr = self.send(b.at[3, cut:], b.at[4, cut:], self.right)
        self.pl = self.send(b.at[3, cut:], b.at[5, cut:], self.left)

    def sideways(self):
        b = self.buf
        self.r.wait_recv()
        self.fr = self.send(b.at[1, :128], b.at[6, :128], self.right)
        self.l.wait_recv()
        self.fl = self.send(b.at[2, 128:], b.at[6, 128:], self.left)

    def over(self):
        b, cut = self.buf, self.cut
        self.yl = self.send(b.at[1, :cut], b.at[4, :cut], self.across)
        self.yr = self.send(b.at[2, :cut], b.at[5, :cut], self.across)

    def far(self):
        b, cut, mid = self.buf, self.cut, self.mid
        self.pr.wait_recv()
        self.fpr = self.send(b.at[4, cut:mid], b.at[7, cut:mid], self.right)
        self.pl.wait_recv()
        self.fpl = self.send(b.at[5, mid:], b.at[7, mid:], self.left)

    def sides(self):
        self.yl.wait_recv()
        self.yr.wait_recv()

    def opposite(self):
        b, cut = self.buf, self.cut
        self.fr.wait_recv()
        self.yo = self.send(b.at[6, :cut], b.at[7, :cut], self.across)
        self.fl.wait_recv()

    def last(self):
        self.yo.wait_recv()
        self.fpr.wait_recv()
        self.fpl.wait_recv()


def kernel(
    rows_hbm, hid, w, low, mid, wj, cot,
    joined, grad,
    rows_in, dr, hid_all, w4, low_all, mid_all, pq, drecv, drecv2, zr, pr, hp, hx, high, ordered, sel, wjv,
    sb, rb, ys, yr2, cot_all, relay, send_sems, recv_sems, pair_send, pair_recv, over_send,
    over_recv, ring_send, ring_recv, high_send, high_recv, swap_send, swap_recv, local, grad_sems,
):
    x, yl, z, yh, c = (lax.axis_index(a) for a in AXES)
    right, left = (mod4(x + 1), yl, z, yh, c), (mod4(x - 1), yl, z, yh, c)
    across = (x, 1 - yl, z, yh, c)
    up, down = (x, yl, mod4(z + 1), yh, c), (x, yl, mod4(z - 1), yh, c)
    far_y, core = (x, yl, z, 1 - yh, c), (x, yl, z, yh, 1 - c)
    between = (x, 1 - yl, z, 1 - yh, c)
    far_z = (x, yl, mod4(z + 2), yh, c)

    barrier = pltpu.get_barrier_semaphore()
    partners = (right, left, across, between, up, down, far_z, far_y, core)
    for to in partners:
        pl.semaphore_signal(barrier, inc=1, device_id=to, device_id_type=MESH)
    pl.semaphore_wait(barrier, len(partners))
    copies = Copies(send_sems, recv_sems)
    quarter = w4.shape[2]
    half = 2 * quarter
    nlocal = [0]

    def load(src, dst):
        k = nlocal[0]
        nlocal[0] += 1
        copy = pltpu.make_async_copy(src, dst, local.at[k])
        copy.start()
        return copy

    def cb(dz, y, core_at):
        return cot_all.at[mod4(z + dz) * 4 + y * 2 + core_at]

    own_cot = cb(0, yh, c)
    cot_between = copies.send(cot, relay, between)
    hidden = RowGather(copies, hid_all, hid, right, left, across, 96)
    hidden.own_over()
    hidden.own()
    loads = [load(hid, hid_all.at[0])]
    for j in range(4):
        at = pl.multiple_of(lax.rem(c + (1 if j < 2 else 0), 2) * half + (j % 2) * quarter, quarter)
        loads.append(load(w.at[:, pl.ds(at, quarter)], w4.at[j]))
    cot_up, cot_down, to_core = copies.send(cot, own_cot, up), copies.send(cot, own_cot, down), []
    to_core.append(copies.send(cot, own_cot, core))
    late = [load(cot, own_cot), load(low, low_all.at[0]), load(mid, mid_all.at[0])]
    late.append(load(rows_hbm, rows_in))
    depth = low.shape[1]
    for k in range(3):
        for d in range(2):
            late.append(
                load(wj.at[k, :, d * half : (d + 1) * half], wjv.at[d, k * depth : (k + 1) * depth])
            )
    for copy in loads:
        copy.wait()

    def project(first, stop, which):
        def body(i, _):
            s, j = first + i // 2, i % 2
            pq[which, s, j] = jnp.dot(hid_all[s], w4[which * 2 + j], preferred_element_type=F32)
            return 0

        lax.fori_loop(0, 2 * (stop - first), body, 0)

    to_pair = {}

    def product(first, stop):
        project(first, stop, 0)
        for s in range(first, stop):
            to_pair[s] = copies.send(pq.at[0, s], drecv.at[s], core)
        project(first, stop, 1)

    def pair_sum(first, stop):
        for s in range(first, stop):
            to_pair[s].wait_recv()

        def body(s, _):
            pq[1, s] = pq[1, s] + drecv[s]
            return 0

        lax.fori_loop(first, stop, body, 0)

    def chunk(k):
        return pl.ds(pl.multiple_of(mod4(k) * 64, 64), 64)

    class Sums:
        def __init__(self, group, first, stop):
            self.group, self.first, self.stop = group, first, stop

        def start(self, step):
            f, t = self.first, self.stop
            self.moved = (
                copies.send(pq.at[1, f:t, 0, chunk(z - 1 - step)], zr.at[step, 0, f:t], up),
                copies.send(pq.at[1, f:t, 1, chunk(z + 1 + step)], zr.at[step, 1, f:t], down),
            )

        def add(self, step):
            f, t = self.first, self.stop
            for d, at in ((0, chunk(z - 2 - step)), (1, chunk(z + 2 + step))):
                self.moved[d].wait_recv()
                pq[1, f:t, d, at] = pq[1, f:t, d, at] + zr[step, d, f:t]

        def advance(self, step):
            self.add(step)
            self.start(step + 1)

        def cross(self):
            self.add(2)
            f, t, g = self.first, self.stop, self.group
            self.pair = pltpu.make_async_remote_copy(
                src_ref=pq.at[1, f:t, :, chunk(z)],
                dst_ref=pr.at[yh, f:t],
                send_sem=pair_send.at[g],
                recv_sem=pair_recv.at[g, yh],
                device_id=(x, 1 - yl, z, yl, c),
                device_id_type=MESH,
            )
            self.pair.start()
            self.over = pltpu.make_async_remote_copy(
                src_ref=hp.at[f:t],
                dst_ref=hp.at[f:t],
                send_sem=over_send.at[g],
                recv_sem=over_recv.at[g],
                device_id=across,
                device_id_type=MESH,
            )

        def total(self):
            f, t, g = self.first, self.stop, self.group

            @pl.when(yh != yl)
            def _():
                for n in range(2):
                    pltpu.make_async_remote_copy(
                        src_ref=pr.at[n, f:t],
                        dst_ref=pr.at[n, f:t],
                        send_sem=pair_send.at[g],
                        recv_sem=pair_recv.at[g, n],
                        device_id=across,
                        device_id_type=MESH,
                    ).wait_recv()
                for d in range(2):
                    value = pr[0, f:t, d] + pr[1, f:t, d]
                    hp[f:t, :, d * quarter : (d + 1) * quarter] = value.astype(BF16)
                self.over.start()

        def to_reader(self, n):
            f, t, g = self.first, self.stop, self.group
            src = hp if n == 0 else hx.at[n - 1]
            at = mod4(x + (0, 3, 1, 2)[n])
            copy = pltpu.make_async_remote_copy(
                src_ref=src.at[f:t],
                dst_ref=high.at[f:t, z],
                send_sem=high_send.at[g, n],
                recv_sem=high_recv.at[g, z],
                device_id=(x, yl, at, yh, c),
                device_id_type=MESH,
            )
            return copy, at, src

        def read(self, n):
            f, t = self.first, self.stop
            copy, at, src = self.to_reader(n)
            pl.when(at != z)(copy.start)

            @pl.when(at == z)
            def _():
                high[f:t, z] = src[f:t]

        def ring(self, n, src, dst, to):
            copy = pltpu.make_async_remote_copy(
                src_ref=src,
                dst_ref=dst,
                send_sem=ring_send.at[self.group, n],
                recv_sem=ring_recv.at[self.group, n],
                device_id=to,
                device_id_type=MESH,
            )
            copy.start()
            self.rings.append(copy)

        def publish(self):
            f, t = self.first, self.stop

            @pl.when(yh == yl)
            def _():
                self.over.wait_recv()

            self.rings = []
            self.ring(0, hp.at[f:t], hx.at[0, f:t], right)
            self.ring(1, hp.at[f:t], hx.at[1, f:t], left)
            self.read(0)

        def forward(self):
            f, t = self.first, self.stop
            self.rings[0].wait_recv()
            self.ring(2, hx.at[0, f:t, :32], hx.at[2, f:t, :32], right)
            self.read(1)
            self.rings[1].wait_recv()
            self.ring(3, hx.at[1, f:t, 32:], hx.at[2, f:t, 32:], left)
            self.read(2)

        def finish(self):
            self.rings[2].wait_recv()
            self.rings[3].wait_recv()
            self.read(3)

        def arrive(self):
            f, t, g = self.first, self.stop, self.group
            for i in range(4):
                @pl.when(z != i)
                def _():
                    pltpu.make_async_remote_copy(
                        src_ref=hp.at[f:t],
                        dst_ref=high.at[f:t, i],
                        send_sem=high_send.at[g, 0],
                        recv_sem=high_recv.at[g, i],
                        device_id=core,
                        device_id_type=MESH,
                    ).wait_recv()

        def drain(self):
            self.pair.wait_send()
            pl.when(yh != yl)(self.over.wait_send)
            for copy in self.rings:
                copy.wait_send()
            for n in range(4):
                copy, at, _ = self.to_reader(n)
                pl.when(at != z)(copy.wait_send)

    a, b, e, f = Sums(0, 0, 4), Sums(1, 4, 6), Sums(2, 6, 7), Sums(3, 7, 8)
    groups = (a, b, e, f)

    product(0, 1)
    for copy in late:
        copy.wait()
    cot_half = cot.shape[0] // 2
    ends = []

    def cot_forward(from_down, from_up, y):
        from_down.wait_recv()
        blk = cb(-1, y, c)
        ends.append(copies.send(blk.at[:cot_half], blk.at[:cot_half], up))
        to_core.append(copies.send(blk, blk, core))
        from_up.wait_recv()
        blk = cb(1, y, c)
        ends.append(copies.send(blk.at[cot_half:], blk.at[cot_half:], down))
        to_core.append(copies.send(blk, blk, core))

    for i in range(16):
        lanes = jnp.broadcast_to(rows_in[i : i + 1, :], (128, 128)).astype(F32)
        dr[i * 128 : (i + 1) * 128, :] = lanes.T.astype(jnp.int32)

    def select(row, bx, by):
        rows = dr[pl.ds(row, 256), :]
        lane = lax.broadcasted_iota(jnp.int32, (256, 128), 1)
        for s in range(8):
            base = (mod4(bx + DX[s]) * 2 + lax.rem(by + DY[s], 2)) * 256
            rel = rows - base
            for h in range(2):
                hit = jnp.where(rel == lane + h * 128, 1.0, 0.0).astype(BF16)
                sel[:, s * 256 + h * 128 : s * 256 + (h + 1) * 128] = hit

    wide = 2 * depth

    def order(features, at, first, stop):
        def body(i, _):
            row = pl.multiple_of(i * 256, 256)
            select(row, x, yl)
            ordered[pl.ds(row, 256), at : at + depth] = jnp.dot(
                sel[...], features[...].reshape(2048, depth), preferred_element_type=F32
            ).astype(BF16)
            return 0

        lax.fori_loop(first, stop, body, 0)

    y_cot = cb(0, 1 - yh, c)
    cot_between.wait_recv()
    cot_forward(cot_up, cot_down, yh)

    hidden.partner()
    hidden.sideways()
    hidden.over()
    cot_over = copies.send(relay, y_cot, across)
    lows = RowGather(copies, low_all, low_all.at[0], right, left, across, 32)
    mids = RowGather(copies, mid_all, mid_all.at[0], right, left, across, 32)
    product(1, 4)
    pair_sum(0, 4)
    a.start(0)
    hidden.far()
    lows.own()
    mids.own()
    a.advance(0)
    hidden.sides()
    product(4, 6)
    hidden.opposite()
    lows.own_over()
    mids.own_over()
    pair_sum(4, 6)
    b.start(0)
    a.advance(1)
    product(6, 7)
    b.advance(0)
    pair_sum(6, 7)
    e.start(0)
    a.cross()
    b.advance(1)
    e.advance(0)
    hidden.last()
    product(7, 8)
    b.cross()
    pair_sum(7, 8)
    f.start(0)
    lows.sideways()
    lows.partner()
    e.advance(1)
    f.advance(0)
    mids.sideways()
    mids.partner()
    e.cross()
    f.advance(1)
    f.cross()
    cot_over.wait_recv()
    ycot_up, ycot_down = copies.send(y_cot, y_cot, up), copies.send(y_cot, y_cot, down)
    to_core.append(copies.send(y_cot, y_cot, core))
    a.total()
    a.publish()
    lows.over()
    lows.opposite()
    lows.far()
    b.total()
    b.publish()
    mids.over()
    mids.opposite()
    mids.far()
    a.forward()
    e.total()
    e.publish()
    b.forward()
    f.total()
    f.publish()
    a.finish()
    lows.sides()
    lows.last()
    cot_forward(ycot_up, ycot_down, 1 - yh)
    e.forward()
    b.finish()
    order(low_all, 0, 0, 4)
    f.forward()
    e.finish()
    order(low_all, 0, 4, 8)
    f.finish()
    mids.sides()
    mids.last()
    order(mid_all, depth, 0, 8)
    for copy in ends:
        copy.wait_recv()
    for y in (yh, 1 - yh):
        blk = cb(2, y, c)
        to_core.append(copies.send(blk, blk, core))
    for copy in to_core:
        copy.wait_recv()

    def saving(n, slot, part):
        row = pl.multiple_of(lax.rem(n, depth // 256) * 256, 256)
        return pltpu.make_async_copy(
            drecv.at[slot * 2 + part // 2, part % 2],
            grad.at[n // (depth // 256), pl.ds(row, 256), part * quarter : (part + 1) * quarter],
            grad_sems.at[n, part],
        )

    def gradient(first, stop):
        def body(n, _):
            slot = lax.rem(n, 4)
            features = ordered[:, pl.ds(pl.multiple_of(n * 256, 256), 256)]
            value = lax.dot_general(
                features,
                cot_all[...].reshape(features.shape[0], 2 * half),
                (((0,), (0,)), ((), ())),
                preferred_element_type=F32,
            )
            for part in range(4):
                at = part * quarter
                drecv[slot * 2 + part // 2, part % 2] = value[:, at : at + quarter]
            for part in range(4):
                saving(n, slot, part).start()
            return 0

        lax.fori_loop(first, stop, body, 0)

    def saved(first, stop):
        for n in range(first, stop):
            for part in range(4):
                saving(n, n % 4, part).wait()

    for g in groups:
        g.arrive()
    for g in groups:
        g.drain()
    copies.drain()

    ring_at = (mod4(z - 1), mod4(z + 1), mod4(z + 2), z)

    def order_high(i):
        def body(n, _):
            row = pl.multiple_of(ring_at[i] * 512 + n * 256, 256)
            select(row, z, yh)
            ordered[pl.ds(row, 256), wide:] = jnp.dot(
                sel[...], high[...].reshape(2048, half), preferred_element_type=F32
            ).astype(BF16)
            return 0

        lax.fori_loop(0, 2, body, 0)

    paired = {}

    def join(i, d):
        def part(which, _):
            side = lax.rem(c + 1 - which, 2)
            at = pl.multiple_of(ring_at[i] * 512 + side * 128, 128)
            rows = jnp.concatenate(
                [ordered[pl.ds(at, 128), :], ordered[pl.ds(at + 256, 128), :]], axis=0
            )
            value = jnp.dot(rows, wjv[d], preferred_element_type=F32)
            pq[which, 2 * i + d, 0] = value[:, :quarter]
            pq[which, 2 * i + d, 1] = value[:, quarter:]

            @pl.when(which == 0)
            def _():
                swap(i, d).start()

            return 0

        lax.fori_loop(0, 2, part, 0)
        paired[i, d] = swap(i, d)

    def swap(i, d):
        return pltpu.make_async_remote_copy(
            src_ref=pq.at[0, 2 * i + d],
            dst_ref=drecv2.at[2 * i + d],
            send_sem=swap_send.at[i, d],
            recv_sem=swap_recv.at[i, d],
            device_id=core,
            device_id_type=MESH,
        )

    streams = (1 - yh, yh)
    turns = ((0, 2, 1, 3), (1, 2, 0, 3))

    def both(i, d, st):
        at = pl.ds(pl.multiple_of(streams[st] * 128, 128), 128)
        return pq[1, 2 * i + d, :, at] + drecv2[2 * i + d, :, at]

    moving = {}

    def turn(step, d, st):
        value = both(turns[d][step], d, st)
        if step:
            moving[step - 1, d, st].wait_recv()
            value = value + rb[d, step - 1, st].astype(F32)
        if step < 3:
            sb[d, step, st] = value.astype(BF16)
            to = up if d == 0 else down
            moving[step, d, st] = copies.send(sb.at[d, step, st], rb.at[d, step, st], to)
        return value

    order_high(0)
    join(0, 0)
    order_high(1)
    join(1, 1)
    paired[0, 0].wait_recv()
    turn(0, 0, 0)
    turn(0, 0, 1)
    paired[1, 1].wait_recv()
    turn(0, 1, 0)
    turn(0, 1, 1)
    order_high(2)
    join(2, 0)
    join(2, 1)
    join(1, 0)
    paired[2, 0].wait_recv()
    paired[2, 1].wait_recv()
    for st in range(2):
        for d in range(2):
            turn(1, d, st)
    join(0, 1)
    order_high(3)
    join(3, 0)
    join(3, 1)
    paired[1, 0].wait_recv()
    paired[0, 1].wait_recv()
    for st in range(2):
        for d in range(2):
            turn(2, d, st)
    gradient(2, 4)
    paired[3, 0].wait_recv()
    paired[3, 1].wait_recv()
    for d in range(2):
        ys[d] = turn(3, d, 0).astype(ys.dtype)
    last = copies.send(ys, yr2, far_y)
    final = [turn(3, d, 1) for d in range(2)]
    gradient(0, 2)
    saved(0, 2)
    gradient(4, 6)
    last.wait_recv()
    for d in range(2):
        value = (final[d] + yr2[d].astype(F32)).astype(BF16)
        for h in range(2):
            at = d * half + h * quarter
            joined[:, at : at + quarter] = value[h]
    copies.drain()
    for copy in paired.values():
        copy.wait_send()
    saved(2, 6)


def deliver(joined, grad, joined_out, grad_out, joined_buf, grad_buf, sems):
    blocks = [(joined, joined_buf, joined_out)]
    rows = grad.shape[1] // 4
    for k in range(3):
        for h in range(4):
            at = (k, pl.ds(h * rows, rows))
            blocks.append((grad.at[at], grad_buf.at[at], grad_out.at[at]))
    loads = [pltpu.make_async_copy(s, b, sems.at[0, n]) for n, (s, b, _) in enumerate(blocks)]
    stores = [pltpu.make_async_copy(b, o, sems.at[1, n]) for n, (_, b, o) in enumerate(blocks)]
    for copy in loads:
        copy.start()
    for copy, store in zip(loads, stores):
        copy.wait()
        store.start()
    for store in stores:
        store.wait()


def on_device(hidden, down_weight, low_feat, mid_feat, draft_rows, join_weight, cotangent):
    tokens = draft_rows.shape[0]
    units, width = down_weight.shape
    depth = low_feat.shape[1]
    half, quarter = width // 2, width // 4
    rows = draft_rows.reshape(tokens // 128, 128)
    anywhere = pl.BlockSpec(memory_space=pl.ANY)
    vmem = pltpu.VMEM
    joined, grad = pl.pallas_call(
        kernel,
        out_shape=(
            jax.ShapeDtypeStruct((128, width), BF16),
            jax.ShapeDtypeStruct((3, depth, width), F32),
        ),
        in_specs=[anywhere] * 7,
        out_specs=(pl.BlockSpec(memory_space=vmem), anywhere),
        scratch_shapes=[
            vmem((tokens // 128, 128), jnp.int32),
            vmem((tokens, 128), jnp.int32),
            vmem((8, 256, units), BF16),
            vmem((4, units, quarter), BF16),
            vmem((8, 256, depth), BF16),
            vmem((8, 256, depth), BF16),
            vmem((2, 8, 2, 256, quarter), F32),
            vmem((8, 2, 256, quarter), F32),
            vmem((8, 2, 256, quarter), F32),
            vmem((3, 2, 8, 64, quarter), F32),
            vmem((2, 8, 2, 64, quarter), F32),
            vmem((8, 64, half), BF16),
            vmem((3, 8, 64, half), BF16),
            vmem((8, 4, 64, half), BF16),
            vmem((tokens, 3 * depth), BF16),
            vmem((256, tokens), BF16),
            vmem((2, 3 * depth, half), BF16),
            vmem((2, 3, 2, 2, 128, quarter), BF16),
            vmem((2, 3, 2, 2, 128, quarter), BF16),
            vmem((2, 2, 128, quarter), BF16),
            vmem((2, 2, 128, quarter), BF16),
            vmem((16, 128, width), BF16),
            vmem((128, width), BF16),
            pltpu.SemaphoreType.DMA((120,)),
            pltpu.SemaphoreType.DMA((120,)),
            pltpu.SemaphoreType.DMA((4,)),
            pltpu.SemaphoreType.DMA((4, 2)),
            pltpu.SemaphoreType.DMA((4,)),
            pltpu.SemaphoreType.DMA((4,)),
            pltpu.SemaphoreType.DMA((4, 4)),
            pltpu.SemaphoreType.DMA((4, 4)),
            pltpu.SemaphoreType.DMA((4, 4)),
            pltpu.SemaphoreType.DMA((4, 4)),
            pltpu.SemaphoreType.DMA((4, 2)),
            pltpu.SemaphoreType.DMA((4, 2)),
            pltpu.SemaphoreType.DMA((24,)),
            pltpu.SemaphoreType.DMA((6, 4)),
        ],
        compiler_params=pltpu.CompilerParams(
            collective_id=0, has_side_effects=True, vmem_limit_bytes=66_000_000
        ),
    )(rows, hidden, down_weight, low_feat, mid_feat, join_weight, cotangent)
    return pl.pallas_call(
        deliver,
        out_shape=(
            jax.ShapeDtypeStruct(joined.shape, BF16),
            jax.ShapeDtypeStruct(grad.shape, F32),
        ),
        in_specs=[anywhere] * 2,
        out_specs=(anywhere, anywhere),
        scratch_shapes=[
            vmem(joined.shape, BF16),
            vmem(grad.shape, F32),
            pltpu.SemaphoreType.DMA((2, 13)),
        ],
    )(joined, grad)


def solution(mesh):
    finer = Mesh(mesh.devices.reshape(4, 2, 4, 2, 2), AXES)
    in_specs = (
        P(ROWS, TENSOR),
        P(TENSOR, ROWS),
        P(ROWS, TENSOR),
        P(ROWS, TENSOR),
        P(),
        P(None, TENSOR, ROWS),
        P(TENSOR, ROWS),
    )
    out_specs = (P(TENSOR, ROWS), P(None, TENSOR, ROWS))
    return jax.shard_map(
        on_device, mesh=finer, in_specs=in_specs, out_specs=out_specs, check_vma=False
    )
```
